256 devices in a mesh: rows: 16 (over z_lo, x), cols: 16 (over y, z_hi, core).
Axes of the slice: x: 4, y: 4, z: 8 (z_hi: 2, z_lo: 4; z = z_hi * 4 + z_lo), core: 2. Of those that a mesh axis runs over, the one named last changes fastest.
Arguments:
- kernel_hat: bfloat16 [2, 256, 512, 4096], P(None, 'rows', 'cols'), may hold values from -0.5 to 0.5
- coefficients: float32 [128, 512], P(None, 'cols'), may hold values from -6 to 6
- wave_speed_sq: float32 [4096, 4096], P('rows', 'cols'), may hold values from 1 to 4
- wet_mask: int32 [4096, 4096], P('rows', 'cols'), may hold values 0 or 1
- boundary_cell: int32 [4096], replicated, may hold values from 0 to 4095, each once
- height: float32 [4096, 4096], P('rows', 'cols'), may hold values from -3 to 3
- flux_x: float32 [4096, 4096], P('rows', 'cols'), may hold values from -3 to 3
- flux_y: float32 [4096, 4096], P('rows', 'cols'), may hold values from -3 to 3
Outputs:
- boundary_series: float32 [128, 4096], P('rows', 'cols')
- height_out: float32 [4096, 4096], P('rows', 'cols')
- flux_x_out: float32 [4096, 4096], P('rows', 'cols')
- flux_y_out: float32 [4096, 4096], P('rows', 'cols')
The draws below stay inside these ranges and needn't reach their ends.
Inputs may be any that keep to these rules, and one draw needn't show every extreme that they name: `boundary_cell`: each of the 4096 boundary points names a different grid column, so each column is named by exactly one point.
All inputs are finite; a program needn't handle non-finite values. No bound on the sum of `wet_mask` on one device may be relied on, other than what follows from the above.
Results may differ from the reference program's by a relative error of at most 0.0029.
Values sent between devices are 32-bit elements; how exact they have to be, the bound alone decides.
A program may use at most 64 MiB of HBM per device.

```python
import math
import jax
import jax.numpy as jnp
from jax import lax

NT = 128
SRC = 512
NF = 256
OBS = 4096
NR = 4096
NC = 4096


def touch_ends(array, own_key, least, top_value):
    longest = array.shape.index(max(array.shape))
    spots = []
    for shift in (0, 1):
        where = [jax.random.randint(jax.random.fold_in(own_key, axis), (), 0, length) for axis, length in enumerate(array.shape)]
        where[longest] = (where[longest] + shift) % array.shape[longest]
        spots.append(tuple(where))
    return array.at[spots[0]].set(least).at[spots[1]].set(top_value)


def block_scale(rng, extent, shards, least, largest):
    factor_of, own = 1.0, jax.random.fold_in(rng, 6)
    for axis_at, shards_of in shards:
        steps = jnp.exp(jax.random.uniform(jax.random.fold_in(own, axis_at), (shards_of,), jnp.float32, least / len(shards), largest / len(shards)))
        factor_of = factor_of * jnp.repeat(steps, extent[axis_at] // shards_of).reshape([-1 if axis == axis_at else 1 for axis in range(len(extent))])
    return factor_of


def scatter_about(key, shape, width, reach, cuts=(), kind=jnp.bfloat16):
    values = width * jax.random.normal(key, shape, jnp.float32)
    if cuts:
        values = values * block_scale(key, shape, cuts, -0.22, 0.18)
    return jnp.clip(values, -reach, reach).astype(kind)


def setup_inputs(seed: int = 0) -> dict:
    keys = jax.random.split(jax.random.key(seed), 9)
    return {
        "kernel_hat": scatter_about(keys[0], (2, NF, SRC, OBS), (SRC // 4) ** -0.5, 0.5, ((1, 16), (2, 16))),
        "coefficients": scatter_about(keys[1], (NT, SRC), 1.0, 6.0, ((1, 16),), jnp.float32),
        "wave_speed_sq": jnp.clip(jnp.exp(math.log(4.0) - 1.3862944 * jax.random.uniform(keys[2], (NR, NC), jnp.float32) ** block_scale(keys[2], (NR, NC), ((0, 16), (1, 16)), -0.2, 0.2)), 1.0, 4.0),
        "wet_mask": touch_ends((jax.random.randint(keys[3], (NR, NC), 0, 4) < 3).astype(jnp.int32), jax.random.fold_in(keys[3], 1), 0, 1),
        "boundary_cell": jax.random.permutation(keys[4], OBS).astype(jnp.int32),
        "height": scatter_about(keys[5], (NR, NC), 0.5, 3.0, ((0, 16), (1, 16)), jnp.float32),
        "flux_x": scatter_about(keys[6], (NR, NC), 0.5, 3.0, ((0, 16), (1, 16)), jnp.float32),
        "flux_y": scatter_about(keys[7], (NR, NC), 0.5, 3.0, ((0, 16), (1, 16)), jnp.float32),
    }


STEP_RATIO = 0.25

def neighbours(values, along_dim):
    if along_dim == 1:
        return (values[1:-1, :-1], values[1:-1, 1:])
    return (values[:-1, 1:-1], values[1:, 1:-1])

def face_fluxes(surface, along, across, speed_sq, celerity, wet, along_dim):
    left_surf, right_surf = neighbours(surface, along_dim)
    left_along, right_along = neighbours(along, along_dim)
    left_across, right_across = neighbours(across, along_dim)
    left_sq, right_sq = neighbours(speed_sq, along_dim)
    left_speed, right_speed = neighbours(celerity, along_dim)
    left_wet, right_wet = neighbours(wet, along_dim)
    opened = left_wet * right_wet
    damping = 0.25 * (left_speed + right_speed)
    mass_flux = opened * (0.5 * (left_along + right_along) - damping * (right_surf - left_surf))
    momentum = opened * (0.5 * (left_sq * left_surf + right_sq * right_surf) - damping * (right_along - left_along))
    shear_flux = opened * (-damping * (right_across - left_across))
    return (mass_flux, momentum, shear_flux)

def advance(surface, along_x, along_y, speed_sq, wet):
    celerity = jnp.sqrt(speed_sq)
    mass_x, momentum_x, shear_x = face_fluxes(surface, along_x, along_y, speed_sq, celerity, wet, 1)
    mass_y, momentum_y, shear_y = face_fluxes(surface, along_y, along_x, speed_sq, celerity, wet, 0)
    interior_wet = wet[1:-1, 1:-1]

    def update(values, flux_cols, flux_rows):
        change = flux_cols[:, 1:] - flux_cols[:, :-1] + (flux_rows[1:] - flux_rows[:-1])
        return interior_wet * (values[1:-1, 1:-1] - STEP_RATIO * change)
    return (update(surface, mass_x, mass_y), update(along_x, momentum_x, shear_y), update(along_y, shear_x, momentum_y))

def reference(kernel_hat, coefficients, wave_speed_sq, wet_mask, boundary_cell, height, flux_x, flux_y):
    spectrum = jnp.fft.fft(coefficients, n=NF, axis=0)
    coef_re = lax.optimization_barrier(jnp.real(spectrum).astype(jnp.bfloat16)).astype(jnp.float32)
    coef_im = lax.optimization_barrier(jnp.imag(spectrum).astype(jnp.bfloat16)).astype(jnp.float32)
    high = lax.Precision.HIGHEST

    def one_frequency(index):
        kern_re = lax.dynamic_index_in_dim(kernel_hat[0], index, 0, keepdims=False).astype(jnp.float32)
        kern_im = lax.dynamic_index_in_dim(kernel_hat[1], index, 0, keepdims=False).astype(jnp.float32)
        row_re = lax.dynamic_index_in_dim(coef_re, index, 0, keepdims=False)
        row_im = lax.dynamic_index_in_dim(coef_im, index, 0, keepdims=False)
        spec_re = jnp.dot(row_re, kern_re, precision=high) - jnp.dot(row_im, kern_im, precision=high)
        spec_im = jnp.dot(row_im, kern_re, precision=high) + jnp.dot(row_re, kern_im, precision=high)
        return (spec_re, spec_im)
    spec_re, spec_im = lax.map(one_frequency, jnp.arange(NF, dtype=jnp.int32))
    times = jnp.arange(NT, dtype=jnp.int32)
    freqs = jnp.arange(NF, dtype=jnp.int32)
    phase = (times[:, None] * freqs[None, :] % NF).astype(jnp.float32) * (2.0 * math.pi / NF)
    series = (jnp.dot(jnp.cos(phase), spec_re, precision=high) - jnp.dot(jnp.sin(phase), spec_im, precision=high)) / NF
    latest = series[NT - 2:]
    ghost = jnp.zeros((2, NC), jnp.float32).at[:, boundary_cell].set(latest)
    wet = wet_mask.astype(jnp.float32)
    speed_pad = jnp.pad(wave_speed_sq, 1).at[-1].set(1.0)
    wet_pad = jnp.pad(wet, 1).at[-1].set(1.0)
    surface, along_x, along_y = (height, flux_x, flux_y)
    for step in range(2):
        surf_pad = jnp.pad(surface, 1).at[-1, 1:-1].set(ghost[step])
        surface, along_x, along_y = advance(surf_pad, jnp.pad(along_x, 1), jnp.pad(along_y, 1), speed_pad, wet_pad)
    return (series, surface, along_x, along_y)
```

```python
import functools
import math

import jax
import jax.numpy as jnp
import numpy as np
from jax import lax
from jax.experimental import pallas as pl
from jax.experimental.pallas import tpu as pltpu
from jax.sharding import PartitionSpec as P

MESH = pl.DeviceIdType.MESH
GROUP = 8
X, Y, Z_LOW, Z_HIGH, CORES = 4, 4, 4, 2, 2
Y_ORDER = (2, 1, 3, 0)
BARRIER_AFTER = 3
EDGE = 8
LANE = 128
F32 = jnp.float32
BF16 = jnp.bfloat16


def tables(freq_total, steps, row_devs):
    freq = np.arange(freq_total)
    time = np.arange(steps)
    phase = 2.0 * math.pi * (np.outer(freq, time) % freq_total) / freq_total
    cos = np.cos(phase).reshape(row_devs, -1, GROUP, steps)
    sin = np.sin(phase).reshape(row_devs, -1, GROUP, steps)
    both = np.concatenate([cos, -sin], axis=2).reshape(row_devs, -1, steps)
    forward = both.astype(np.float32)
    inverse = np.swapaxes(both, 1, 2) / freq_total
    high = inverse.astype(np.float32).astype(jnp.bfloat16)
    low = (inverse - high.astype(np.float64)).astype(np.float32).astype(jnp.bfloat16)
    return forward, np.concatenate([high, high, low], axis=2)


def split(value):
    high = value.astype(BF16)
    return high, value - high.astype(F32)


def faces(speed, wet, dim):
    ahead = speed.shape[dim] - 1
    opened = wet * pltpu.roll(wet, ahead, dim)
    return 0.5 * opened, opened * (0.25 * (speed + pltpu.roll(speed, ahead, dim)))


def step_once(surf, qx, qy, speed_sq, wet, face_x, face_y):
    energy = speed_sq * surf
    change = []
    for dim, along, across, (half, damp) in ((1, qx, qy, face_x), (0, qy, qx, face_y)):
        ahead = surf.shape[dim] - 1
        later = lambda v: pltpu.roll(v, ahead, dim)
        mass = half * (along + later(along)) - damp * (later(surf) - surf)
        momentum = half * (energy + later(energy)) - damp * (later(along) - along)
        shear = -damp * (later(across) - across)
        change.append([f - pltpu.roll(f, 1, dim) for f in (mass, momentum, shear)])
    (mass_x, mom_x, shear_x), (mass_y, mom_y, shear_y) = change
    return (
        wet * (surf - 0.25 * (mass_x + mass_y)),
        wet * (qx - 0.25 * (mom_x + shear_y)),
        wet * (qy - 0.25 * (shear_x + mom_y)),
    )


def kernel(
    n_rows, n_cols,
    kern_hbm, coef_hbm, sq_hbm, wet_hbm, cell_hbm, surf_hbm, qx_hbm, qy_hbm, fwd_hbm, inv_hbm,
    series_buf, out_buf,
    kern, coef, fwd, inv, cells, pad, wet_int, corner, strip_out, strip_in,
    part, core_in, y_out, y_in, z_out, z_in, whole_buf, whole_in,
    late_part, late_in, late_out, edge_in, last_out, last_in, latest_buf, mid, chosen_buf,
    local_sem, kern_sem, core_recv, halo_send, halo_recv, late_send, send_sem, recv_sem,
):
    row = lax.axis_index("rows")
    col = lax.axis_index("cols")
    x, z_low = lax.rem(row, X), row // X
    y, z_high, core = col // (Z_HIGH * CORES), lax.rem(col // CORES, Z_HIGH), lax.rem(col, CORES)
    z = z_high * Z_LOW + z_low
    freqs, src = kern.shape[2:4]
    groups = freqs // GROUP
    tall, wide = surf_hbm.shape
    obs = cells.shape[1]
    points = obs // n_cols
    per_y = obs // Y
    own_steps = series_buf.shape[0]
    has_n, has_s = row > 0, row < n_rows - 1
    has_w, has_e = col > 0, col < n_cols - 1
    at_edge = row == n_rows - 1

    def column(y_at, z_high_at, core_at):
        return (y_at * Z_HIGH + z_high_at) * CORES + core_at

    inputs = [
        pltpu.make_async_copy(coef_hbm, coef, local_sem.at[0]),
        pltpu.make_async_copy(fwd_hbm.at[row], fwd, local_sem.at[1]),
        pltpu.make_async_copy(inv_hbm.at[row], inv, local_sem.at[2]),
        pltpu.make_async_copy(surf_hbm, pad.at[0, :tall, :wide], local_sem.at[3]),
        pltpu.make_async_copy(qx_hbm, pad.at[1, :tall, :wide], local_sem.at[4]),
        pltpu.make_async_copy(qy_hbm, pad.at[2, :tall, :wide], local_sem.at[5]),
        pltpu.make_async_copy(sq_hbm, pad.at[3, :tall, :wide], local_sem.at[6]),
        pltpu.make_async_copy(wet_hbm, wet_int, local_sem.at[7]),
        pltpu.make_async_copy(cell_hbm, cells, local_sem.at[8]),
    ]
    for copy in inputs[:3]:
        copy.start()
    chunks = []
    for i, dy in enumerate(Y_ORDER):
        at = pl.multiple_of(lax.rem(y + dy, Y) * per_y, per_y)
        for p in range(2):
            copy = pltpu.make_async_copy(
                kern_hbm.at[p, :, :, pl.ds(at, per_y)], kern.at[i, p], kern_sem.at[i, p]
            )
            copy.start()
            chunks.append(copy)
    for copy in inputs[3:]:
        copy.start()

    diagonals = [
        (has_n & has_w, -1, -1), (has_n & has_e, -1, 1),
        (has_s & has_w, 1, -1), (has_s & has_e, 1, 1),
    ]
    plane = [(dy, dc) for dy in range(Y) for dc in range(CORES) if dy or dc]
    barrier = pltpu.get_barrier_semaphore()

    def greet(to):
        pl.semaphore_signal(barrier, 1, device_id=to, device_id_type=MESH)

    def beside_me(dy, dc):
        return (row, column(lax.rem(y + dy, Y), z_high, lax.rem(core + dc, CORES)))

    partner_z = (row, column(y, 1 - z_high, core))
    partner_core = (row, column(y, z_high, 1 - core))
    for k in range(1, n_rows):
        greet((lax.rem(row + k, n_rows), col))
    greet(partner_z)
    for dy, dc in plane:
        greet(beside_me(dy, dc))
    sides = [(has_w, 0, -1), (has_e, 0, 1)] + diagonals
    for exists, dr, dc in sides:
        @pl.when(exists)
        def _(dr=dr, dc=dc):
            greet((row + dr, col + dc))

    @pl.when(at_edge)
    def _():
        for r in range(n_rows - 1):
            greet((r, partner_z[1]))
        for k in range(1, n_cols):
            greet((row, lax.rem(col + k, n_cols)))

    def remote(source, target, send, recv, to):
        return pltpu.make_async_remote_copy(
            src_ref=source, dst_ref=target, send_sem=send, recv_sem=recv,
            device_id=to, device_id_type=MESH,
        )

    def whole_wait(ref, sem):
        return remote(ref, ref, sem, sem, partner_core)

    inputs[0].wait()
    inputs[1].wait()
    spectrum = lax.dot_general(
        fwd[...], coef[...], (((1,), (1,)), ((), ())),
        precision=lax.Precision.HIGHEST, preferred_element_type=F32,
    )
    spread = jnp.where(
        lax.rem(lax.broadcasted_iota(jnp.int32, (src, GROUP * src), 1), src)
        == lax.broadcasted_iota(jnp.int32, (src, GROUP * src), 0), 1.0, 0.0
    ).astype(BF16)
    shape = (2 * GROUP, GROUP * src)
    own_block = (
        lax.broadcasted_iota(jnp.int32, shape, 1) // src
        == lax.rem(lax.broadcasted_iota(jnp.int32, shape, 0), GROUP)
    )
    lefts = []
    for g in range(groups):
        mine = spectrum[g * 2 * GROUP:(g + 1) * 2 * GROUP]
        turned = jnp.concatenate([-mine[GROUP:], mine[:GROUP]], axis=0)
        for value in (mine, turned):
            tiled = jnp.dot(value.astype(BF16), spread, preferred_element_type=F32)
            lefts.append(jnp.where(own_block, tiled, 0.0).astype(BF16))

    def send_chunk(i):
        remote(
            part.at[i, 1 - core], core_in.at[i], send_sem.at[0], core_recv.at[i], partner_core
        ).start()
        for k, (dy, dc) in enumerate(plane):
            if dy == Y_ORDER[i]:
                remote(
                    late_part.at[i, lax.rem(core + dc, CORES)], late_in.at[k],
                    send_sem.at[1], recv_sem.at[1], beside_me(dy, dc),
                ).start()

    inputs[2].wait()
    late_rows = inv[inv.shape[0] - 2 * GROUP:]
    for i in range(Y):
        chunks[2 * i].wait()
        chunks[2 * i + 1].wait()
        totals = []
        for g in range(groups):
            total = None
            for p in range(2):
                right = kern[i, p, pl.ds(g * GROUP, GROUP)].reshape(GROUP * src, per_y)
                term = jnp.dot(lefts[2 * g + p], right, preferred_element_type=F32)
                total = term if total is None else total + term
            totals.append(total)
        total = jnp.concatenate(totals, axis=0)
        high, low = split(total)
        late = jnp.dot(
            late_rows, jnp.concatenate([high, low.astype(BF16), high], axis=0),
            preferred_element_type=F32,
        )[2 * GROUP - 2:]
        for h in range(Z_HIGH):
            for c in range(CORES):
                at = (h * CORES + c) * points
                part[i, c, h] = total[:, at:at + points]
                late_part[i, c, h] = late[:, at:at + points]
        if i == BARRIER_AFTER:
            pl.semaphore_wait(
                barrier,
                n_rows - 1 + 1 + len(plane) + jnp.where(at_edge, n_cols - 1, 1)
                + sum(exists.astype(jnp.int32) for exists, _, _ in sides),
            )
            for j in range(i + 1):
                send_chunk(j)
        elif i > BARRIER_AFTER:
            send_chunk(i)

    for copy in inputs[3:8]:
        copy.wait()
    pad[4, :tall, :wide] = wet_int[...].astype(F32)
    lane = lax.broadcasted_iota(jnp.int32, (tall, LANE), 1)
    packed = jnp.zeros((tall, LANE), F32)
    for k in range(5):
        first, last = pad[k, :tall, :LANE], pad[k, :tall, wide - LANE:wide]
        at = 2 * k
        moved = first if at == 0 else pltpu.roll(first, at, 1)
        packed = jnp.where((lane >= at) & (lane < at + 2), moved, packed)
        at = 16 + 2 * k
        packed = jnp.where(
            (lane >= at) & (lane < at + 2), pltpu.roll(last, at + 2, 1), packed
        )
    strip_out[...] = packed.T[:32]

    for i in range(Y):
        whole_wait(core_in.at[i], core_recv.at[i]).wait_recv()
        if Y_ORDER[i]:
            y_out[i] = part[i, core] + core_in[i]
            remote(
                y_out.at[i], y_in.at[i], send_sem.at[2], recv_sem.at[2],
                (row, column(lax.rem(y + Y_ORDER[i], Y), z_high, core)),
            ).start()

    north = (lax.rem(row + n_rows - 1, n_rows), col)
    south = (lax.rem(row + 1, n_rows), col)
    west = (row, lax.rem(col + n_cols - 1, n_cols))
    east = (row, lax.rem(col + 1, n_cols))
    top, bottom = pl.ds(0, EDGE), pl.ds(tall - EDGE, EDGE)
    south_halo, north_halo = pl.ds(tall, EDGE), pl.ds(tall + EDGE, EDGE)
    body = pl.ds(0, wide)

    def halo(source, target, i, to):
        return remote(source, target, halo_send.at[i], halo_recv.at[i], to)

    moves = [
        (has_n, has_s, halo(pad.at[:, top, body], pad.at[:, south_halo, body], 0, north)),
        (has_s, has_n, halo(pad.at[:, bottom, body], pad.at[:, north_halo, body], 1, south)),
        (has_w, has_e, halo(strip_out.at[pl.ds(0, 16)], strip_in.at[pl.ds(16, 16)], 2, west)),
        (has_e, has_w, halo(strip_out.at[pl.ds(16, 16)], strip_in.at[pl.ds(0, 16)], 3, east)),
    ]
    for i, (exists, dr, dc) in enumerate(diagonals):
        rows_at = top if dr < 0 else bottom
        cols_at = pl.ds(0, LANE) if dc < 0 else pl.ds(wide - LANE, LANE)
        to = (lax.rem(row + dr + n_rows, n_rows), lax.rem(col + dc + n_cols, n_cols))
        moves.append((
            exists, diagonals[3 - i][0],
            halo(pad.at[:, rows_at, cols_at], corner.at[i], 4 + i, to),
        ))
    for exists, _, copy in moves:
        @pl.when(exists)
        def _(copy=copy):
            copy.start()

    whole_wait(late_in, recv_sem.at[1]).wait_recv()
    late = late_part[Y - 1, core]
    for k in range(len(plane)):
        late = late + late_in[k]
    late_out[...] = late
    for h in range(Z_HIGH):
        @pl.when(jnp.logical_not(at_edge & (z_high == h)))
        def _(h=h):
            ahead = lax.rem(h * Z_LOW + Z_LOW - 1 - z + Z_LOW * Z_HIGH, Z_LOW * Z_HIGH)
            slot = lax.max(ahead * X + X - 1 - x - 1, 0)
            remote(
                late_out.at[h], edge_in.at[slot], late_send.at[h], recv_sem.at[3],
                (n_rows - 1, column(y, h, core)),
            ).start()

    whole_wait(y_in, recv_sem.at[2]).wait_recv()
    value = part[Y - 1, core] + core_in[Y - 1]
    for i in range(Y - 1):
        value = value + y_in[i]
    z_out[...] = value
    z_copy = remote(z_out.at[1 - z_high], z_in, send_sem.at[3], recv_sem.at[4], partner_z)
    z_copy.start()

    for i, (_, arrives, copy) in enumerate(moves):
        @pl.when(arrives)
        def _(copy=copy):
            copy.wait_recv()

        @pl.when(jnp.logical_not(arrives))
        def _(i=i):
            if i == 0:
                pad[:, south_halo, body] = jnp.zeros((5, EDGE, wide), F32)
            elif i == 1:
                pad[:, north_halo, body] = jnp.zeros((5, EDGE, wide), F32)
            elif i == 2:
                strip_in[pl.ds(16, 16)] = jnp.zeros((16, tall), F32)
            elif i == 3:
                strip_in[pl.ds(0, 16)] = jnp.zeros((16, tall), F32)
            else:
                corner[i - 4] = jnp.zeros((5, EDGE, LANE), F32)

    beside = jnp.concatenate([strip_in[...], jnp.zeros((LANE - 32, tall), F32)], axis=0).T
    near = lax.broadcasted_iota(jnp.int32, (EDGE, LANE), 1) < LANE // 2
    for k in range(5):
        pad[k, :tall, wide:] = jnp.where(
            lane < LANE // 2,
            pltpu.roll(beside, LANE - 16 - 2 * k, 1),
            pltpu.roll(beside, LANE - 2 - 2 * k, 1),
        )
        pad[k, tall:tall + EDGE, wide:] = jnp.where(near, corner[0, k], corner[1, k])
        pad[k, tall + EDGE:, wide:] = jnp.where(near, corner[2, k], corner[3, k])

    @pl.when(at_edge)
    def _():
        pad[3:5, tall:tall + 1, :] = jnp.ones((2, 1, wide + LANE), F32)

    def first_step():
        wet, speed_sq = pad[4], pad[3]
        speed = jnp.sqrt(speed_sq)
        face_x, face_y = faces(speed, wet, 1), faces(speed, wet, 0)
        new = step_once(pad[0], pad[1], pad[2], speed_sq, wet, face_x, face_y)
        for k in range(3):
            mid[k] = new[k]

    def second_step():
        wet, speed_sq = pad[4], pad[3]
        speed = jnp.sqrt(speed_sq)
        face_x, face_y = faces(speed, wet, 1), faces(speed, wet, 0)
        new = step_once(mid[0], mid[1], mid[2], speed_sq, wet, face_x, face_y)
        for k in range(3):
            out_buf[k] = new[k][:tall, :wide]

    first_step()

    whole_wait(z_in, recv_sem.at[4]).wait_recv()
    high, low = split(z_out[z_high] + z_in[...])
    whole = jnp.dot(
        inv[...], jnp.concatenate([high, low.astype(BF16), high], axis=0),
        preferred_element_type=F32,
    )
    whole_buf[...] = whole
    for k in range(1, n_rows):
        to = lax.rem(row + k, n_rows)
        remote(
            whole_buf.at[pl.ds(pl.multiple_of(to * own_steps, own_steps), own_steps)],
            whole_in.at[k - 1], send_sem.at[4], recv_sem.at[5], (to, col),
        ).start()

    inputs[8].wait()
    span = wide + LANE

    @pl.when(at_edge)
    def _():
        whole_wait(edge_in, recv_sem.at[3]).wait_recv()
        value = late_out[z_high]
        for k in range(Z_LOW * Z_HIGH * X - 1):
            value = value + edge_in[k]
        last_out[...] = value
        latest_buf[col] = value
        for k in range(1, n_cols):
            remote(
                last_out, last_in.at[k - 1], send_sem.at[5], recv_sem.at[6],
                (row, lax.rem(col + k, n_cols)),
            ).start()
        place = lax.broadcasted_iota(jnp.int32, (span, obs), 0)
        place = jnp.where(place >= wide + LANE // 2, place - span, place) + col * wide
        chosen_buf[...] = jnp.where(place == cells[...], 1.0, 0.0).astype(BF16)

    second_step()

    whole_wait(whole_in, recv_sem.at[5]).wait_recv()
    value = whole_buf[pl.ds(pl.multiple_of(row * own_steps, own_steps), own_steps)]
    for k in range(1, n_rows):
        value = value + whole_in[k - 1]
    series_buf[...] = value

    @pl.when(at_edge)
    def _():
        whole_wait(last_in, recv_sem.at[6]).wait_recv()
        for k in range(1, n_cols):
            latest_buf[lax.rem(col + n_cols - k, n_cols)] = last_in[k - 1]
        latest = jnp.concatenate([latest_buf[d] for d in range(n_cols)], axis=1)
        high, rest = split(latest)
        middle, rest = split(rest)
        parts = jnp.concatenate([high.astype(F32), middle.astype(F32), rest, rest], axis=0)
        picked = lax.dot_general(
            parts.astype(BF16), chosen_buf[...], (((1,), (1,)), ((), ())),
            preferred_element_type=F32,
        )
        picked = picked[0:2] + picked[2:4] + picked[4:6]
        base = tall - 2 * EDGE
        part_rows = pl.ds(base, 3 * EDGE)
        at_ghost = lax.broadcasted_iota(jnp.int32, (3 * EDGE, span), 0) == 2 * EDGE
        ghosts = [
            jnp.broadcast_to(picked[k:k + 1], (3 * EDGE, span)) for k in range(2)
        ]
        wet, speed_sq = pad[4, part_rows], pad[3, part_rows]
        speed = jnp.sqrt(speed_sq)
        face_x, face_y = faces(speed, wet, 1), faces(speed, wet, 0)
        surf = jnp.where(at_ghost, ghosts[0], pad[0, part_rows])
        surf, qx, qy = step_once(
            surf, pad[1, part_rows], pad[2, part_rows], speed_sq, wet, face_x, face_y
        )
        surf = jnp.where(at_ghost, ghosts[1], surf)
        qx = jnp.where(at_ghost, 0.0, qx)
        qy = jnp.where(at_ghost, 0.0, qy)
        new = step_once(surf, qx, qy, speed_sq, wet, face_x, face_y)
        for k in range(3):
            out_buf[k, tall - EDGE:] = new[k][EDGE:2 * EDGE, :wide]

    for exists, _, copy in moves:
        @pl.when(exists)
        def _(copy=copy):
            copy.wait_send()
    for ref, sem in (
        (part.at[:, 0], send_sem.at[0]), (late_in, send_sem.at[1]), (y_in, send_sem.at[2]),
        (z_in, send_sem.at[3]), (whole_in, send_sem.at[4]),
    ):
        whole_wait(ref, sem).wait_send()
    for h in range(Z_HIGH):
        @pl.when(jnp.logical_not(at_edge & (z_high == h)))
        def _(h=h):
            whole_wait(late_out.at[h], late_send.at[h]).wait_send()

    @pl.when(at_edge)
    def _():
        whole_wait(last_in, send_sem.at[5]).wait_send()


def write_out(series, fields, series_hbm, surf_hbm, qx_hbm, qy_hbm, sems):
    copies = [pltpu.make_async_copy(series, series_hbm, sems.at[3])]
    for k, target in enumerate((surf_hbm, qx_hbm, qy_hbm)):
        copies.append(pltpu.make_async_copy(fields.at[k], target, sems.at[k]))
    for copy in copies:
        copy.start()
    for copy in copies:
        copy.wait()


def on_device(n_rows, n_cols, kernel_hat, coefficients, wave_speed_sq, wet_mask, boundary_cell, height, flux_x, flux_y):
    _, freqs, src, obs = kernel_hat.shape
    steps = coefficients.shape[0]
    tall, wide = height.shape
    points = obs // n_cols
    own_steps = steps // n_rows
    span = wide + LANE
    forward, inverse = tables(freqs * n_rows, steps, n_rows)
    dma = pltpu.SemaphoreType.DMA
    anywhere = pl.BlockSpec(memory_space=pltpu.HBM)
    in_vmem = pl.BlockSpec(memory_space=pltpu.VMEM)
    series, fields = pl.pallas_call(
        functools.partial(kernel, n_rows, n_cols),
        out_shape=(
            pltpu.VMEM((own_steps, points), F32),
            pltpu.VMEM((3, tall, wide), F32),
        ),
        in_specs=[anywhere] * 10,
        out_specs=(in_vmem,) * 2,
        scratch_shapes=[
            pltpu.VMEM((Y, 2, freqs, src, obs // Y), BF16),
            pltpu.VMEM((src, steps), F32),
            pltpu.VMEM(forward.shape[1:], F32),
            pltpu.VMEM(inverse.shape[1:], BF16),
            pltpu.VMEM((1, obs), jnp.int32),
            pltpu.VMEM((5, tall + 2 * EDGE, span), F32),
            pltpu.VMEM((tall, wide), jnp.int32),
            pltpu.VMEM((4, 5, EDGE, LANE), F32),
            pltpu.VMEM((32, tall), F32),
            pltpu.VMEM((32, tall), F32),
            pltpu.VMEM((Y, CORES, Z_HIGH, 2 * freqs, points), F32),
            pltpu.VMEM((Y, Z_HIGH, 2 * freqs, points), F32),
            pltpu.VMEM((Y - 1, Z_HIGH, 2 * freqs, points), F32),
            pltpu.VMEM((Y - 1, Z_HIGH, 2 * freqs, points), F32),
            pltpu.VMEM((Z_HIGH, 2 * freqs, points), F32),
            pltpu.VMEM((2 * freqs, points), F32),
            pltpu.VMEM((steps, points), F32),
            pltpu.VMEM((n_rows - 1, own_steps, points), F32),
            pltpu.VMEM((Y, CORES, Z_HIGH, 2, points), F32),
            pltpu.VMEM((Y * CORES - 1, Z_HIGH, 2, points), F32),
            pltpu.VMEM((Z_HIGH, 2, points), F32),
            pltpu.VMEM((X * Z_LOW * Z_HIGH - 1, 2, points), F32),
            pltpu.VMEM((2, points), F32),
            pltpu.VMEM((n_cols - 1, 2, points), F32),
            pltpu.VMEM((n_cols, 2, points), F32),
            pltpu.VMEM((3, tall + 2 * EDGE, span), F32),
            pltpu.VMEM((span, obs), BF16),
            dma((9,)),
            dma((Y, 2)),
            dma((Y,)),
            dma((8,)),
            dma((8,)),
            dma((Z_HIGH,)),
            dma((6,)),
            dma((7,)),
        ],
        compiler_params=pltpu.CompilerParams(
            collective_id=0, has_side_effects=True, vmem_limit_bytes=60 * 1024 * 1024
        ),
    )(
        kernel_hat, coefficients.T, wave_speed_sq, wet_mask, boundary_cell.reshape(1, obs),
        height, flux_x, flux_y, jnp.asarray(forward), jnp.asarray(inverse),
    )
    return pl.pallas_call(
        write_out,
        out_shape=(
            jax.ShapeDtypeStruct((own_steps, points), F32),
            jax.ShapeDtypeStruct((tall, wide), F32),
            jax.ShapeDtypeStruct((tall, wide), F32),
            jax.ShapeDtypeStruct((tall, wide), F32),
        ),
        in_specs=[in_vmem] * 2,
        out_specs=(anywhere,) * 4,
        scratch_shapes=[dma((4,))],
        compiler_params=pltpu.CompilerParams(vmem_limit_bytes=4 * 1024 * 1024),
    )(series, fields)


def solution(mesh):
    n_rows, n_cols = mesh.shape["rows"], mesh.shape["cols"]
    return jax.shard_map(
        functools.partial(on_device, n_rows, n_cols),
        mesh=mesh,
        in_specs=(
            P(None, "rows", "cols", None),
            P(None, "cols"),
            P("rows", "cols"),
            P("rows", "cols"),
            P(),
            P("rows", "cols"),
            P("rows", "cols"),
            P("rows", "cols"),
        ),
        out_specs=(P("rows", "cols"), P("rows", "cols"), P("rows", "cols"), P("rows", "cols")),
        check_vma=False,
    )
```

```python
import functools
import math

import jax
import jax.numpy as jnp
import numpy as np
from jax import lax
from jax.experimental import pallas as pl
from jax.experimental.pallas import tpu as pltpu
from jax.sharding import PartitionSpec as P

MESH = pl.DeviceIdType.MESH
GROUP = 8
X, Y, Z_LOW, Z_HIGH, CORES = 4, 4, 4, 2, 2
Y_ORDER = (2, 1, 3, 0)
BARRIER_AFTER = 2
EDGE = 8
LANE = 128
F32 = jnp.float32
BF16 = jnp.bfloat16


def halves(table):
    high = table.astype(np.float32).astype(jnp.bfloat16)
    low = (table - high.astype(np.float64)).astype(np.float32).astype(jnp.bfloat16)
    return np.concatenate([high, high, low], axis=2)


def tables(freq_total, steps, row_devs):
    freq = np.arange(freq_total)
    time = np.arange(steps)
    phase = 2.0 * math.pi * (np.outer(freq, time) % freq_total) / freq_total
    cos = np.cos(phase).reshape(row_devs, -1, GROUP, steps)
    sin = np.sin(phase).reshape(row_devs, -1, GROUP, steps)
    both = np.concatenate([cos, -sin], axis=2).reshape(row_devs, -1, steps)
    forward = both.astype(np.float32)
    inverse = np.swapaxes(both, 1, 2) / freq_total
    four = np.swapaxes(both.reshape(row_devs // X, -1, steps), 1, 2) / freq_total
    return forward, halves(inverse[:, steps - 2 * GROUP:]), halves(four)


def split(value):
    high = value.astype(BF16)
    return high, value - high.astype(F32)


def faces(speed, wet, dim):
    ahead = speed.shape[dim] - 1
    opened = wet * pltpu.roll(wet, ahead, dim)
    return 0.5 * opened, opened * (0.25 * (speed + pltpu.roll(speed, ahead, dim)))


def step_once(surf, qx, qy, speed_sq, wet, face_x, face_y):
    energy = speed_sq * surf
    change = []
    for dim, along, across, (half, damp) in ((1, qx, qy, face_x), (0, qy, qx, face_y)):
        ahead = surf.shape[dim] - 1
        later = lambda v: pltpu.roll(v, ahead, dim)
        mass = half * (along + later(along)) - damp * (later(surf) - surf)
        momentum = half * (energy + later(energy)) - damp * (later(along) - along)
        shear = -damp * (later(across) - across)
        change.append([f - pltpu.roll(f, 1, dim) for f in (mass, momentum, shear)])
    (mass_x, mom_x, shear_x), (mass_y, mom_y, shear_y) = change
    return (
        wet * (surf - 0.25 * (mass_x + mass_y)),
        wet * (qx - 0.25 * (mom_x + shear_y)),
        wet * (qy - 0.25 * (shear_x + mom_y)),
    )


def kernel(
    n_rows, n_cols,
    kern_hbm, coef_hbm, sq_hbm, wet_hbm, cell_hbm, surf_hbm, qx_hbm, qy_hbm, fwd_hbm, tail_hbm, inv_hbm,
    series_buf, out_buf,
    kern, coef, fwd, tail, inv, cells, pad, wet_int, corner, strip_out, strip_in,
    part, core_in, plane_out, plane_in, spec_buf, whole_buf, whole_in,
    late_part, late_in, late_out, edge_in, mid, chosen_buf,
    local_sem, kern_sem, core_recv, halo_send, halo_recv, send_sem, recv_sem,
):
    row = lax.axis_index("rows")
    col = lax.axis_index("cols")
    x, z_low = lax.rem(row, X), row // X
    y, z_high, core = col // (Z_HIGH * CORES), lax.rem(col // CORES, Z_HIGH), lax.rem(col, CORES)
    z = z_high * Z_LOW + z_low
    freqs, src = kern.shape[2:4]
    groups = freqs // GROUP
    tall, wide = surf_hbm.shape
    obs = cells.shape[1]
    points = obs // n_cols
    per_y = obs // Y
    own_steps = series_buf.shape[0]
    has_n, has_s = row > 0, row < n_rows - 1
    has_w, has_e = col > 0, col < n_cols - 1
    at_edge = row == n_rows - 1

    inputs = [
        pltpu.make_async_copy(coef_hbm, coef, local_sem.at[0]),
        pltpu.make_async_copy(fwd_hbm.at[row], fwd, local_sem.at[1]),
        pltpu.make_async_copy(tail_hbm.at[row], tail, local_sem.at[2]),
        pltpu.make_async_copy(surf_hbm, pad.at[0, :tall, :wide], local_sem.at[3]),
        pltpu.make_async_copy(qx_hbm, pad.at[1, :tall, :wide], local_sem.at[4]),
        pltpu.make_async_copy(qy_hbm, pad.at[2, :tall, :wide], local_sem.at[5]),
        pltpu.make_async_copy(sq_hbm, pad.at[3, :tall, :wide], local_sem.at[6]),
        pltpu.make_async_copy(wet_hbm, wet_int, local_sem.at[7]),
        pltpu.make_async_copy(inv_hbm.at[z_low], inv, local_sem.at[8]),
        pltpu.make_async_copy(cell_hbm, cells, local_sem.at[9]),
    ]
    for copy in inputs[:3]:
        copy.start()
    chunks = []
    for i, dy in enumerate(Y_ORDER):
        at = pl.multiple_of(lax.rem(y + dy, Y) * per_y, per_y)
        for p in range(2):
            copy = pltpu.make_async_copy(
                kern_hbm.at[p, :, :, pl.ds(at, per_y)], kern.at[i, p], kern_sem.at[i, p]
            )
            copy.start()
            chunks.append(copy)

    diagonals = [
        (has_n & has_w, -1, -1), (has_n & has_e, -1, 1),
        (has_s & has_w, 1, -1), (has_s & has_e, 1, 1),
    ]
    plane = [
        (dy, dx, dc) for dy in range(Y) for dx in range(X) for dc in range(CORES) if dy or dx or dc
    ]
    depth = Z_LOW * Z_HIGH
    home = x // Z_HIGH == z_high
    barrier = pltpu.get_barrier_semaphore()

    def greet(to):
        pl.semaphore_signal(barrier, 1, device_id=to, device_id_type=MESH)

    def device(x_at, y_at, z_at, core_at):
        return (
            lax.rem(z_at, Z_LOW) * X + x_at,
            (y_at * Z_HIGH + z_at // Z_LOW) * CORES + core_at,
        )

    def in_plane(dy, dx, dc):
        return device(lax.rem(x + dx, X), lax.rem(y + dy, Y), z, lax.rem(core + dc, CORES))

    partner_core = device(x, y, z, 1 - core)

    @pl.when(at_edge)
    def _():
        for dz in range(1, depth):
            greet(device(x, y, lax.rem(z + dz, depth), core))
    for dz in (4, 3, 5, 2, 6, 1, 7):
        for half in range(2):
            greet(device(z_high * 2 + half, y, lax.rem(z + dz, depth), core))
    for half in range(2):
        @pl.when(x != z_high * 2 + half)
        def _(half=half):
            greet(device(z_high * 2 + half, y, z, core))
    for dy, dx, dc in plane:
        greet(in_plane(dy, dx, dc))
    sides = [(has_n, -1, 0), (has_s, 1, 0), (has_w, 0, -1), (has_e, 0, 1)] + diagonals
    for exists, dr, dc in sides:
        @pl.when(exists)
        def _(dr=dr, dc=dc):
            greet((row + dr, col + dc))
    for copy in inputs[3:]:
        copy.start()

    def remote(source, target, send, recv, to):
        return pltpu.make_async_remote_copy(
            src_ref=source, dst_ref=target, send_sem=send, recv_sem=recv,
            device_id=to, device_id_type=MESH,
        )

    def whole_wait(ref, sem):
        return remote(ref, ref, sem, sem, partner_core)

    inputs[0].wait()
    inputs[1].wait()
    spectrum = lax.dot_general(
        fwd[...], coef[...], (((1,), (1,)), ((), ())),
        precision=lax.Precision.HIGHEST, preferred_element_type=F32,
    )
    spread = jnp.where(
        lax.rem(lax.broadcasted_iota(jnp.int32, (src, GROUP * src), 1), src)
        == lax.broadcasted_iota(jnp.int32, (src, GROUP * src), 0), 1.0, 0.0
    ).astype(BF16)
    shape = (2 * GROUP, GROUP * src)
    own_block = (
        lax.broadcasted_iota(jnp.int32, shape, 1) // src
        == lax.rem(lax.broadcasted_iota(jnp.int32, shape, 0), GROUP)
    )
    lefts = []
    for g in range(groups):
        mine = spectrum[g * 2 * GROUP:(g + 1) * 2 * GROUP]
        turned = jnp.concatenate([-mine[GROUP:], mine[:GROUP]], axis=0)
        for value in (mine, turned):
            tiled = jnp.dot(value.astype(BF16), spread, preferred_element_type=F32)
            lefts.append(jnp.where(own_block, tiled, 0.0).astype(BF16))

    def send_chunk(i):
        remote(
            part.at[i, 1 - core], core_in.at[i], send_sem.at[0], core_recv.at[i], partner_core
        ).start()
        for k, (dy, dx, dc) in enumerate(plane):
            if dy == Y_ORDER[i]:
                remote(
                    late_part.at[i, lax.rem(core + dc, CORES), lax.rem(x + dx, X)], late_in.at[k],
                    send_sem.at[1], recv_sem.at[0], in_plane(dy, dx, dc),
                ).start()

    inputs[2].wait()
    for i in range(Y):
        chunks[2 * i].wait()
        chunks[2 * i + 1].wait()
        totals = []
        for g in range(groups):
            total = None
            for p in range(2):
                right = kern[i, p, pl.ds(g * GROUP, GROUP)].reshape(GROUP * src, per_y)
                term = jnp.dot(lefts[2 * g + p], right, preferred_element_type=F32)
                total = term if total is None else total + term
            totals.append(total)
        total = jnp.concatenate(totals, axis=0)
        high, low = split(total)
        late = jnp.dot(
            tail[...], jnp.concatenate([high, low.astype(BF16), high], axis=0),
            preferred_element_type=F32,
        )[2 * GROUP - 2:]
        for h in range(Z_HIGH):
            for c in range(CORES):
                for half in range(2):
                    at = (h * CORES + c) * points + half * LANE
                    part[i, c, 2 * h + half] = total[:, at:at + LANE]
                    late_part[i, c, 2 * h + half] = late[:, at:at + LANE]
        if i == BARRIER_AFTER:
            pl.semaphore_wait(
                barrier,
                len(plane) + 2 * depth - home.astype(jnp.int32)
                + jnp.where(x == X - 1, 2 - at_edge.astype(jnp.int32), 0)
                + sum(exists.astype(jnp.int32) for exists, _, _ in sides),
            )
            for j in range(i + 1):
                send_chunk(j)
        elif i > BARRIER_AFTER:
            send_chunk(i)

    for copy in inputs[3:8]:
        copy.wait()
    pad[4, :tall, :wide] = wet_int[...].astype(F32)
    lane = lax.broadcasted_iota(jnp.int32, (tall, LANE), 1)
    packed = jnp.zeros((tall, LANE), F32)
    for k in range(5):
        first, last = pad[k, :tall, :LANE], pad[k, :tall, wide - LANE:wide]
        at = 2 * k
        moved = first if at == 0 else pltpu.roll(first, at, 1)
        packed = jnp.where((lane >= at) & (lane < at + 2), moved, packed)
        at = 16 + 2 * k
        packed = jnp.where(
            (lane >= at) & (lane < at + 2), pltpu.roll(last, at + 2, 1), packed
        )
    strip_out[...] = packed.T[:32]

    for i in range(Y):
        whole_wait(core_in.at[i], core_recv.at[i]).wait_recv()
        plane_out[i] = part[i, core] + core_in[i]
        for dx in (2, 1, 3, 0):
            if Y_ORDER[i] or dx:
                remote(
                    plane_out.at[i, lax.rem(x + dx, X)], plane_in.at[(i + 1) % Y * X + dx],
                    send_sem.at[2], recv_sem.at[1], in_plane(Y_ORDER[i], dx, 0),
                ).start()

    north = (lax.rem(row + n_rows - 1, n_rows), col)
    south = (lax.rem(row + 1, n_rows), col)
    west = (row, lax.rem(col + n_cols - 1, n_cols))
    east = (row, lax.rem(col + 1, n_cols))
    top, bottom = pl.ds(0, EDGE), pl.ds(tall - EDGE, EDGE)
    south_halo, north_halo = pl.ds(tall, EDGE), pl.ds(tall + EDGE, EDGE)
    body = pl.ds(0, wide)

    def halo(source, target, i, to):
        return remote(source, target, halo_send.at[i], halo_recv.at[i], to)

    moves = [
        (has_n, has_s, halo(pad.at[:, top, body], pad.at[:, south_halo, body], 0, north)),
        (has_s, has_n, halo(pad.at[:, bottom, body], pad.at[:, north_halo, body], 1, south)),
        (has_w, has_e, halo(strip_out.at[pl.ds(0, 16)], strip_in.at[pl.ds(16, 16)], 2, west)),
        (has_e, has_w, halo(strip_out.at[pl.ds(16, 16)], strip_in.at[pl.ds(0, 16)], 3, east)),
    ]
    for i, (exists, dr, dc) in enumerate(diagonals):
        rows_at = top if dr < 0 else bottom
        cols_at = pl.ds(0, LANE) if dc < 0 else pl.ds(wide - LANE, LANE)
        to = (lax.rem(row + dr + n_rows, n_rows), lax.rem(col + dc + n_cols, n_cols))
        moves.append((
            exists, diagonals[3 - i][0],
            halo(pad.at[:, rows_at, cols_at], corner.at[i], 4 + i, to),
        ))
    for exists, _, copy in moves:
        @pl.when(exists)
        def _(copy=copy):
            copy.start()

    whole_wait(late_in, recv_sem.at[0]).wait_recv()
    late = late_part[Y - 1, core, x]
    for k in range(len(plane)):
        late = late + late_in[k]
    late_out[...] = late
    block = ((y * Z_HIGH + x // 2) * CORES + core) * 2 + lax.rem(x, 2)
    blocks = obs // LANE
    for k in range(n_cols):
        def _(k=k):
            remote(
                late_out, edge_in.at[z * blocks + block], send_sem.at[3], recv_sem.at[2],
                (n_rows - 1, lax.rem(col + k, n_cols)),
            ).start()
        if k:
            _()
        else:
            pl.when(jnp.logical_not(at_edge))(_)

    @pl.when(at_edge)
    def _():
        edge_in[z * blocks + block] = late

    others = plane_in.at[pl.ds(1, X * Y - 1)]
    whole_wait(others, recv_sem.at[1]).wait_recv()
    for dx in range(X):
        value = plane_out[Y - 1, x] if dx == 0 else plane_in[dx]
        for i in range(Y - 1):
            value = value + plane_in[(i + 1) * X + dx]
        spec_buf[lax.rem(x + X - dx, X)] = value
    inputs[8].wait()
    high, low = split(spec_buf[...].reshape(X * 2 * freqs, LANE))
    whole = jnp.dot(
        inv[...], jnp.concatenate([high, low.astype(BF16), high], axis=0),
        preferred_element_type=F32,
    )
    whole_buf[...] = whole
    z_base = x // 2 * Z_LOW
    own_half = lax.rem(x, 2) * depth
    for k in range(n_rows):
        def _(k=k):
            to = lax.rem(row + k, n_rows)
            z_to = z_base + to // X
            remote(
                whole_buf.at[pl.ds(pl.multiple_of(to * own_steps, own_steps), own_steps)],
                whole_in.at[own_half + lax.rem(z_to - z + depth, depth)],
                send_sem.at[4], recv_sem.at[3], device(lax.rem(to, X), y, z_to, core),
            ).start()
        if k:
            _()
        else:
            pl.when(jnp.logical_not(home))(_)

    @pl.when(home)
    def _():
        whole_in[own_half] = whole_buf[
            pl.ds(pl.multiple_of(row * own_steps, own_steps), own_steps)
        ]

    for i, (_, arrives, copy) in enumerate(moves):
        @pl.when(arrives)
        def _(copy=copy):
            copy.wait_recv()

        @pl.when(jnp.logical_not(arrives))
        def _(i=i):
            if i == 0:
                pad[:, south_halo, body] = jnp.zeros((5, EDGE, wide), F32)
            elif i == 1:
                pad[:, north_halo, body] = jnp.zeros((5, EDGE, wide), F32)
            elif i == 2:
                strip_in[pl.ds(16, 16)] = jnp.zeros((16, tall), F32)
            elif i == 3:
                strip_in[pl.ds(0, 16)] = jnp.zeros((16, tall), F32)
            else:
                corner[i - 4] = jnp.zeros((5, EDGE, LANE), F32)

    beside = jnp.concatenate([strip_in[...], jnp.zeros((LANE - 32, tall), F32)], axis=0).T
    near = lax.broadcasted_iota(jnp.int32, (EDGE, LANE), 1) < LANE // 2
    for k in range(5):
        pad[k, :tall, wide:] = jnp.where(
            lane < LANE // 2,
            pltpu.roll(beside, LANE - 16 - 2 * k, 1),
            pltpu.roll(beside, LANE - 2 - 2 * k, 1),
        )
        pad[k, tall:tall + EDGE, wide:] = jnp.where(near, corner[0, k], corner[1, k])
        pad[k, tall + EDGE:, wide:] = jnp.where(near, corner[2, k], corner[3, k])

    @pl.when(at_edge)
    def _():
        pad[3:5, tall:tall + 1, :] = jnp.ones((2, 1, wide + LANE), F32)

    def first_step():
        wet, speed_sq = pad[4], pad[3]
        speed = jnp.sqrt(speed_sq)
        face_x, face_y = faces(speed, wet, 1), faces(speed, wet, 0)
        new = step_once(pad[0], pad[1], pad[2], speed_sq, wet, face_x, face_y)
        for k in range(3):
            mid[k] = new[k]

    def second_step():
        wet, speed_sq = pad[4], pad[3]
        speed = jnp.sqrt(speed_sq)
        face_x, face_y = faces(speed, wet, 1), faces(speed, wet, 0)
        new = step_once(mid[0], mid[1], mid[2], speed_sq, wet, face_x, face_y)
        for k in range(3):
            out_buf[k] = new[k][:tall, :wide]

    first_step()

    inputs[9].wait()
    span = wide + LANE

    @pl.when(at_edge)
    def _():
        place = lax.broadcasted_iota(jnp.int32, (span, obs), 0)
        place = jnp.where(place >= wide + LANE // 2, place - span, place) + col * wide
        chosen_buf[...] = jnp.where(place == cells[...], 1.0, 0.0).astype(BF16)

    second_step()

    @pl.when(home)
    def _():
        whole_wait(whole_in.at[pl.ds(0, 2 * depth - 1)], recv_sem.at[3]).wait_recv()

    @pl.when(jnp.logical_not(home))
    def _():
        whole_wait(whole_in, recv_sem.at[3]).wait_recv()

    for half in range(2):
        value = whole_in[half * depth]
        for k in range(1, depth):
            value = value + whole_in[half * depth + k]
        series_buf[:, half * LANE:(half + 1) * LANE] = value

    @pl.when(at_edge)
    def _():
        whole_wait(edge_in.at[pl.ds(0, depth * blocks - 1)], recv_sem.at[2]).wait_recv()
        total = edge_in[pl.ds(0, blocks)]
        for k in range(1, depth):
            total = total + edge_in[pl.ds(k * blocks, blocks)]
        latest = jnp.concatenate([total[b] for b in range(blocks)], axis=1)
        high, rest = split(latest)
        middle, rest = split(rest)
        parts = jnp.concatenate([high.astype(F32), middle.astype(F32), rest, rest], axis=0)
        picked = lax.dot_general(
            parts.astype(BF16), chosen_buf[...], (((1,), (1,)), ((), ())),
            preferred_element_type=F32,
        )
        picked = picked[0:2] + picked[2:4] + picked[4:6]
        base = tall - 2 * EDGE
        part_rows = pl.ds(base, 3 * EDGE)
        at_ghost = lax.broadcasted_iota(jnp.int32, (3 * EDGE, span), 0) == 2 * EDGE
        ghosts = [
            jnp.broadcast_to(picked[k:k + 1], (3 * EDGE, span)) for k in range(2)
        ]
        wet, speed_sq = pad[4, part_rows], pad[3, part_rows]
        speed = jnp.sqrt(speed_sq)
        face_x, face_y = faces(speed, wet, 1), faces(speed, wet, 0)
        surf = jnp.where(at_ghost, ghosts[0], pad[0, part_rows])
        surf, qx, qy = step_once(
            surf, pad[1, part_rows], pad[2, part_rows], speed_sq, wet, face_x, face_y
        )
        surf = jnp.where(at_ghost, ghosts[1], surf)
        qx = jnp.where(at_ghost, 0.0, qx)
        qy = jnp.where(at_ghost, 0.0, qy)
        new = step_once(surf, qx, qy, speed_sq, wet, face_x, face_y)
        for k in range(3):
            out_buf[k, tall - EDGE:] = new[k][EDGE:2 * EDGE, :wide]

    for exists, _, copy in moves:
        @pl.when(exists)
        def _(copy=copy):
            copy.wait_send()
    for ref, sem in (
        (core_in, send_sem.at[0]), (late_in, send_sem.at[1]),
        (others, send_sem.at[2]),
    ):
        whole_wait(ref, sem).wait_send()

    @pl.when(at_edge)
    def _():
        whole_wait(edge_in.at[pl.ds(0, n_cols - 1)], send_sem.at[3]).wait_send()

    @pl.when(jnp.logical_not(at_edge))
    def _():
        whole_wait(edge_in.at[pl.ds(0, n_cols)], send_sem.at[3]).wait_send()

    @pl.when(home)
    def _():
        whole_wait(whole_in.at[pl.ds(0, 2 * depth - 1)], send_sem.at[4]).wait_send()

    @pl.when(jnp.logical_not(home))
    def _():
        whole_wait(whole_in, send_sem.at[4]).wait_send()


def write_out(series, fields, series_hbm, surf_hbm, qx_hbm, qy_hbm, sems):
    copies = [pltpu.make_async_copy(series, series_hbm, sems.at[3])]
    for k, target in enumerate((surf_hbm, qx_hbm, qy_hbm)):
        copies.append(pltpu.make_async_copy(fields.at[k], target, sems.at[k]))
    for copy in copies:
        copy.start()
    for copy in copies:
        copy.wait()


def on_device(n_rows, n_cols, kernel_hat, coefficients, wave_speed_sq, wet_mask, boundary_cell, height, flux_x, flux_y):
    _, freqs, src, obs = kernel_hat.shape
    steps = coefficients.shape[0]
    tall, wide = height.shape
    points = obs // n_cols
    own_steps = steps // n_rows
    span = wide + LANE
    forward, tail, inverse = tables(freqs * n_rows, steps, n_rows)
    dma = pltpu.SemaphoreType.DMA
    anywhere = pl.BlockSpec(memory_space=pltpu.HBM)
    in_vmem = pl.BlockSpec(memory_space=pltpu.VMEM)
    series, fields = pl.pallas_call(
        functools.partial(kernel, n_rows, n_cols),
        out_shape=(
            pltpu.VMEM((own_steps, points), F32),
            pltpu.VMEM((3, tall, wide), F32),
        ),
        in_specs=[anywhere] * 11,
        out_specs=(in_vmem,) * 2,
        scratch_shapes=[
            pltpu.VMEM((Y, 2, freqs, src, obs // Y), BF16),
            pltpu.VMEM((src, steps), F32),
            pltpu.VMEM(forward.shape[1:], F32),
            pltpu.VMEM(tail.shape[1:], BF16),
            pltpu.VMEM(inverse.shape[1:], BF16),
            pltpu.VMEM((1, obs), jnp.int32),
            pltpu.VMEM((5, tall + 2 * EDGE, span), F32),
            pltpu.VMEM((tall, wide), jnp.int32),
            pltpu.VMEM((4, 5, EDGE, LANE), F32),
            pltpu.VMEM((32, tall), F32),
            pltpu.VMEM((32, tall), F32),
            pltpu.VMEM((Y, CORES, X, 2 * freqs, LANE), F32),
            pltpu.VMEM((Y, X, 2 * freqs, LANE), F32),
            pltpu.VMEM((Y, X, 2 * freqs, LANE), F32),
            pltpu.VMEM((Y * X, 2 * freqs, LANE), F32),
            pltpu.VMEM((X, 2 * freqs, LANE), F32),
            pltpu.VMEM((steps, LANE), F32),
            pltpu.VMEM((2 * Z_LOW * Z_HIGH, own_steps, LANE), F32),
            pltpu.VMEM((Y, CORES, X, 2, LANE), F32),
            pltpu.VMEM((Y * X * CORES - 1, 2, LANE), F32),
            pltpu.VMEM((2, LANE), F32),
            pltpu.VMEM((Z_LOW * Z_HIGH * (obs // LANE), 2, LANE), F32),
            pltpu.VMEM((3, tall + 2 * EDGE, span), F32),
            pltpu.VMEM((span, obs), BF16),
            dma((10,)),
            dma((Y, 2)),
            dma((Y,)),
            dma((8,)),
            dma((8,)),
            dma((5,)),
            dma((4,)),
        ],
        compiler_params=pltpu.CompilerParams(
            collective_id=0, has_side_effects=True, vmem_limit_bytes=60 * 1024 * 1024
        ),
    )(
        kernel_hat, coefficients.T, wave_speed_sq, wet_mask, boundary_cell.reshape(1, obs),
        height, flux_x, flux_y, jnp.asarray(forward), jnp.asarray(tail),
        jnp.asarray(inverse),
    )
    return pl.pallas_call(
        write_out,
        out_shape=(
            jax.ShapeDtypeStruct((own_steps, points), F32),
            jax.ShapeDtypeStruct((tall, wide), F32),
            jax.ShapeDtypeStruct((tall, wide), F32),
            jax.ShapeDtypeStruct((tall, wide), F32),
        ),
        in_specs=[in_vmem] * 2,
        out_specs=(anywhere,) * 4,
        scratch_shapes=[dma((4,))],
        compiler_params=pltpu.CompilerParams(vmem_limit_bytes=4 * 1024 * 1024),
    )(series, fields)


def solution(mesh):
    n_rows, n_cols = mesh.shape["rows"], mesh.shape["cols"]
    return jax.shard_map(
        functools.partial(on_device, n_rows, n_cols),
        mesh=mesh,
        in_specs=(
            P(None, "rows", "cols", None),
            P(None, "cols"),
            P("rows", "cols"),
            P("rows", "cols"),
            P(),
            P("rows", "cols"),
            P("rows", "cols"),
            P("rows", "cols"),
        ),
        out_specs=(P("rows", "cols"), P("rows", "cols"), P("rows", "cols"), P("rows", "cols")),
        check_vma=False,
    )
```

```python
import functools
import math

import jax
import jax.numpy as jnp
import numpy as np
from jax import lax
from jax.experimental import pallas as pl
from jax.experimental.pallas import tpu as pltpu
from jax.sharding import PartitionSpec as P

MESH = pl.DeviceIdType.MESH
GROUP = 8
REACH = 2
X, Y, Z_LOW, Z_HIGH, CORES = 4, 4, 4, 2, 2
Y_ORDER = (2, 1, 3, 0)
BARRIER_AFTER = 1
EDGE = 8
LANE = 128
F32 = jnp.float32
BF16 = jnp.bfloat16


def halves(table):
    high = table.astype(np.float32).astype(jnp.bfloat16)
    low = (table - high.astype(np.float64)).astype(np.float32).astype(jnp.bfloat16)
    return np.concatenate([high, high, low], axis=2)


def tables(freq_total, steps, row_devs):
    freq = np.arange(freq_total)
    time = np.arange(steps)
    phase = 2.0 * math.pi * (np.outer(freq, time) % freq_total) / freq_total
    cos = np.cos(phase).reshape(row_devs, -1, GROUP, steps)
    sin = np.sin(phase).reshape(row_devs, -1, GROUP, steps)
    both = np.concatenate([cos, -sin], axis=2).reshape(row_devs, -1, steps)
    forward = both.astype(np.float32)
    inverse = np.swapaxes(both, 1, 2) / freq_total
    four = np.swapaxes(both.reshape(row_devs // X, -1, steps), 1, 2) / freq_total
    late = halves(inverse[:, steps - 2 * GROUP:]).astype(np.float32)
    late = np.pad(late, ((0, 0), (0, 0), (0, steps - late.shape[2])))
    return np.concatenate([forward, late], axis=1), halves(four)


def split(value):
    high = value.astype(BF16)
    return high, value - high.astype(F32)


def faces(speed_sq, wet):
    speed = 0.0625 * jnp.sqrt(speed_sq)
    found = []
    for dim in (1, 0):
        ahead = wet.shape[dim] - 1
        opened = wet * pltpu.roll(wet, ahead, dim)
        found += [0.125 * opened, opened * (speed + pltpu.roll(speed, ahead, dim))]
    return found


def step_once(surf, qx, qy, speed_sq, wet, face):
    energy = speed_sq * surf
    change = []
    for dim, along, across, half, damp in ((1, qx, qy, *face[:2]), (0, qy, qx, *face[2:])):
        ahead = surf.shape[dim] - 1
        later = lambda v: pltpu.roll(v, ahead, dim)
        along_later = later(along)
        mass = half * (along + along_later) + damp * (surf - later(surf))
        momentum = half * (energy + later(energy)) + damp * (along - along_later)
        shear = damp * (across - later(across))
        change.append([f - pltpu.roll(f, 1, dim) for f in (mass, momentum, shear)])
    (mass_x, mom_x, shear_x), (mass_y, mom_y, shear_y) = change
    return (
        wet * (surf - (mass_x + mass_y)),
        wet * (qx - (mom_x + shear_y)),
        wet * (qy - (shear_x + mom_y)),
    )


def kernel(
    n_rows, n_cols,
    kern_hbm, coef_hbm, sq_hbm, wet_hbm, cell_hbm, surf_hbm, qx_hbm, qy_hbm, fwd_hbm, inv_hbm,
    series_buf, out_buf,
    kern, coef, fwd, inv, cells, pad, wet_int, corner, rows_out, rows_in, strip_out, strip_in,
    part, core_in, plane_out, plane_in, spec_buf, whole_buf, whole_in,
    late_part, late_in, late_out, edge_in, face_buf, mid, chosen_buf,
    local_sem, kern_sem, core_recv, halo_send, halo_recv, send_sem, recv_sem, near_sem, far_sem,
):
    row = lax.axis_index("rows")
    col = lax.axis_index("cols")
    x, z_low = lax.rem(row, X), row // X
    y, z_high, core = col // (Z_HIGH * CORES), lax.rem(col // CORES, Z_HIGH), lax.rem(col, CORES)
    z = z_high * Z_LOW + z_low
    freqs, src = kern.shape[2:4]
    groups = freqs // GROUP
    tall, wide = surf_hbm.shape
    obs = cells.shape[1]
    points = obs // n_cols
    per_y = obs // Y
    own_steps = series_buf.shape[0]
    has_n, has_s = row > 0, row < n_rows - 1
    has_w, has_e = col > 0, col < n_cols - 1
    at_edge = row == n_rows - 1

    inputs = [
        pltpu.make_async_copy(coef_hbm, coef, local_sem.at[0]),
        pltpu.make_async_copy(fwd_hbm.at[row], fwd, local_sem.at[1]),
        pltpu.make_async_copy(surf_hbm, pad.at[0, :tall, :wide], local_sem.at[3]),
        pltpu.make_async_copy(qx_hbm, pad.at[1, :tall, :wide], local_sem.at[4]),
        pltpu.make_async_copy(qy_hbm, pad.at[2, :tall, :wide], local_sem.at[5]),
        pltpu.make_async_copy(sq_hbm, pad.at[3, :tall, :wide], local_sem.at[6]),
        pltpu.make_async_copy(wet_hbm, wet_int, local_sem.at[7]),
        pltpu.make_async_copy(inv_hbm.at[z_low], inv, local_sem.at[2]),
        pltpu.make_async_copy(cell_hbm, cells, local_sem.at[8]),
    ]
    for copy in inputs[:2]:
        copy.start()
    chunks = []
    for i, dy in enumerate(Y_ORDER):
        at = pl.multiple_of(lax.rem(y + dy, Y) * per_y, per_y)
        for p in range(2):
            copy = pltpu.make_async_copy(
                kern_hbm.at[p, :, :, pl.ds(at, per_y)], kern.at[i, p], kern_sem.at[i, p]
            )
            chunks.append(copy)
    for copy in chunks[:2]:
        copy.start()
    pad[:, tall:] = jnp.zeros((5, 2 * EDGE, wide + LANE), F32)
    rows_in[...] = jnp.zeros(rows_in.shape, F32)
    strip_in[...] = jnp.zeros(strip_in.shape, F32)
    corner[...] = jnp.zeros(corner.shape, F32)

    diagonals = [
        (has_n & has_w, -1, -1), (has_n & has_e, -1, 1),
        (has_s & has_w, 1, -1), (has_s & has_e, 1, 1),
    ]
    plane = [
        (dy, dx, dc) for dy in range(Y) for dx in range(X) for dc in range(CORES) if dy or dx or dc
    ]
    depth = Z_LOW * Z_HIGH
    home = x // Z_HIGH == z_high
    barrier = pltpu.get_barrier_semaphore()

    def greet(to):
        pl.semaphore_signal(barrier, 1, device_id=to, device_id_type=MESH)

    def device(x_at, y_at, z_at, core_at):
        return (
            lax.rem(z_at, Z_LOW) * X + x_at,
            (y_at * Z_HIGH + z_at // Z_LOW) * CORES + core_at,
        )

    def in_plane(dy, dx, dc):
        return device(lax.rem(x + dx, X), lax.rem(y + dy, Y), z, lax.rem(core + dc, CORES))

    partner_core = device(x, y, z, 1 - core)

    def in_line(dz):
        return device(x, y, lax.rem(z + dz + depth, depth), core)

    for dz in (2, -2, 1, -1):
        greet(in_line(dz))
    for copy in chunks[2:4]:
        copy.start()
    for dy, dx, dc in plane:
        greet(in_plane(dy, dx, dc))
    for copy in chunks[4:]:
        copy.start()
    for copy in inputs[2:]:
        copy.start()

    def remote(source, target, send, recv, to):
        return pltpu.make_async_remote_copy(
            src_ref=source, dst_ref=target, send_sem=send, recv_sem=recv,
            device_id=to, device_id_type=MESH,
        )

    def whole_wait(ref, sem):
        return remote(ref, ref, sem, sem, partner_core)

    inputs[0].wait()
    inputs[1].wait()
    spectrum = lax.dot_general(
        fwd[:2 * freqs], coef[...], (((1,), (1,)), ((), ())),
        precision=lax.Precision.HIGHEST, preferred_element_type=F32,
    )
    spread = jnp.where(
        lax.rem(lax.broadcasted_iota(jnp.int32, (src, GROUP * src), 1), src)
        == lax.broadcasted_iota(jnp.int32, (src, GROUP * src), 0), 1.0, 0.0
    ).astype(BF16)
    shape = (2 * GROUP, GROUP * src)
    own_block = (
        lax.broadcasted_iota(jnp.int32, shape, 1) // src
        == lax.rem(lax.broadcasted_iota(jnp.int32, shape, 0), GROUP)
    )
    lefts = []
    for g in range(groups):
        mine = spectrum[g * 2 * GROUP:(g + 1) * 2 * GROUP]
        turned = jnp.concatenate([-mine[GROUP:], mine[:GROUP]], axis=0)
        for value in (mine, turned):
            tiled = jnp.dot(value.astype(BF16), spread, preferred_element_type=F32)
            lefts.append(jnp.where(own_block, tiled, 0.0).astype(BF16))

    def send_chunk(i):
        remote(
            part.at[i, 1 - core], core_in.at[i], send_sem.at[0], core_recv.at[i], partner_core
        ).start()
        for k, (dy, dx, dc) in enumerate(plane):
            if dy == Y_ORDER[i]:
                remote(
                    late_part.at[i, lax.rem(core + dc, CORES), lax.rem(x + dx, X)], late_in.at[k],
                    send_sem.at[1], recv_sem.at[0], in_plane(dy, dx, dc),
                ).start()

    tail = fwd[2 * freqs:].astype(BF16)[:, :6 * freqs]
    for i in range(Y):
        chunks[2 * i].wait()
        chunks[2 * i + 1].wait()
        totals = []
        for g in range(groups):
            total = None
            for p in range(2):
                right = kern[i, p, pl.ds(g * GROUP, GROUP)].reshape(GROUP * src, per_y)
                term = jnp.dot(lefts[2 * g + p], right, preferred_element_type=F32)
                total = term if total is None else total + term
            totals.append(total)
        total = jnp.concatenate(totals, axis=0)
        high, low = split(total)
        late = jnp.dot(
            tail, jnp.concatenate([high, low.astype(BF16), high], axis=0),
            preferred_element_type=F32,
        )[2 * GROUP - 2:]
        for h in range(Z_HIGH):
            for c in range(CORES):
                for half in range(2):
                    at = (h * CORES + c) * points + half * LANE
                    part[i, c, 2 * h + half] = total[:, at:at + LANE]
                    late_part[i, c, 2 * h + half] = late[:, at:at + LANE]
        if i == BARRIER_AFTER:
            pl.semaphore_wait(barrier, len(plane) + 4)
            for dz in (2, -2, 1, -1):
                pl.semaphore_signal(
                    near_sem, 1, device_id=in_line(dz), device_id_type=MESH
                )
            for j in range(i + 1):
                send_chunk(j)
        elif i > BARRIER_AFTER:
            send_chunk(i)

    def gather(i):
        whole_wait(core_in.at[i], core_recv.at[i]).wait_recv()
        plane_out[i] = part[i, core] + core_in[i]
        for dx in (2, 1, 3, 0):
            if Y_ORDER[i] or dx:
                remote(
                    plane_out.at[i, lax.rem(x + dx, X)], plane_in.at[(i + 1) % Y * X + dx],
                    send_sem.at[2], recv_sem.at[1], in_plane(Y_ORDER[i], dx, 0),
                ).start()

    gather(0)
    gather(1)
    pl.semaphore_wait(near_sem, 4)
    for dz in (2, -2):
        pl.semaphore_signal(far_sem, 1, device_id=in_line(dz), device_id_type=MESH)
    gather(2)

    for copy in inputs[2:7]:
        copy.wait()
    pad[4, :tall, :wide] = wet_int[...].astype(F32)
    lane = lax.broadcasted_iota(jnp.int32, (tall, LANE), 1)
    packed = jnp.zeros((tall, LANE), F32)
    for k in range(5):
        first, last = pad[k, :tall, :LANE], pad[k, :tall, wide - LANE:wide]
        at = 2 * k
        moved = first if at == 0 else pltpu.roll(first, at, 1)
        packed = jnp.where((lane >= at) & (lane < at + 2), moved, packed)
        at = 16 + 2 * k
        packed = jnp.where(
            (lane >= at) & (lane < at + 2), pltpu.roll(last, at + 2, 1), packed
        )
    strip_out[...] = packed.T[:32]
    rows_out[0] = pad[:, :REACH, :wide]
    rows_out[1] = pad[:, tall - REACH:tall, :wide]

    gather(Y - 1)
    pl.semaphore_wait(far_sem, 2)

    north = (lax.rem(row + n_rows - 1, n_rows), col)
    south = (lax.rem(row + 1, n_rows), col)
    west = (row, lax.rem(col + n_cols - 1, n_cols))
    east = (row, lax.rem(col + 1, n_cols))
    def halo(source, target, i, to):
        return remote(source, target, halo_send.at[i], halo_recv.at[i], to)

    moves = [
        (has_n, has_s, halo(rows_out.at[0], rows_in.at[0], 0, north)),
        (has_s, has_n, halo(rows_out.at[1], rows_in.at[1], 1, south)),
        (has_w, has_e, halo(strip_out.at[pl.ds(0, 16)], strip_in.at[pl.ds(16, 16)], 2, west)),
        (has_e, has_w, halo(strip_out.at[pl.ds(16, 16)], strip_in.at[pl.ds(0, 16)], 3, east)),
    ]
    for i, (exists, dr, dc) in enumerate(diagonals):
        side = 0 if dr < 0 else 1
        cols_at = pl.ds(0, LANE) if dc < 0 else pl.ds(wide - LANE, LANE)
        to = (lax.rem(row + dr + n_rows, n_rows), lax.rem(col + dc + n_cols, n_cols))
        moves.append((
            exists, diagonals[3 - i][0],
            halo(rows_out.at[side, :, :, cols_at], corner.at[i], 4 + i, to),
        ))
    for exists, _, copy in moves:
        @pl.when(exists)
        def _(copy=copy):
            copy.start()

    whole_wait(late_in, recv_sem.at[0]).wait_recv()
    late = late_part[Y - 1, core, x]
    for k in range(len(plane)):
        late = late + late_in[k]
    late_out[...] = late
    block = ((y * Z_HIGH + x // 2) * CORES + core) * 2 + lax.rem(x, 2)
    blocks = obs // LANE
    for k in range(n_cols):
        def _(k=k):
            remote(
                late_out, edge_in.at[z * blocks + block], send_sem.at[3], recv_sem.at[2],
                (n_rows - 1, lax.rem(col + k, n_cols)),
            ).start()
        if k:
            _()
        else:
            pl.when(jnp.logical_not(at_edge))(_)

    @pl.when(at_edge)
    def _():
        edge_in[z * blocks + block] = late

    others = plane_in.at[pl.ds(1, X * Y - 1)]
    whole_wait(others, recv_sem.at[1]).wait_recv()
    for dx in range(X):
        value = plane_out[Y - 1, x] if dx == 0 else plane_in[dx]
        for i in range(Y - 1):
            value = value + plane_in[(i + 1) * X + dx]
        spec_buf[lax.rem(x + X - dx, X)] = value
    inputs[7].wait()
    high, low = split(spec_buf[...].reshape(X * 2 * freqs, LANE))
    whole = jnp.dot(
        inv[...], jnp.concatenate([high, low.astype(BF16), high], axis=0),
        preferred_element_type=F32,
    )
    whole_buf[...] = whole
    z_base = x // 2 * Z_LOW
    own_half = lax.rem(x, 2) * depth
    for k in range(n_rows):
        def _(k=k):
            to = lax.rem(row + k, n_rows)
            z_to = z_base + to // X
            remote(
                whole_buf.at[pl.ds(pl.multiple_of(to * own_steps, own_steps), own_steps)],
                whole_in.at[own_half + lax.rem(z_to - z + depth, depth)],
                send_sem.at[4], recv_sem.at[3], device(lax.rem(to, X), y, z_to, core),
            ).start()
        if k:
            _()
        else:
            pl.when(jnp.logical_not(home))(_)

    @pl.when(home)
    def _():
        whole_in[own_half] = whole_buf[
            pl.ds(pl.multiple_of(row * own_steps, own_steps), own_steps)
        ]

    for _, arrives, copy in moves:
        @pl.when(arrives)
        def _(copy=copy):
            copy.wait_recv()

    beside = jnp.concatenate([strip_in[...], jnp.zeros((LANE - 32, tall), F32)], axis=0).T
    near = lax.broadcasted_iota(jnp.int32, (REACH, LANE), 1) < LANE // 2
    below, above = pl.ds(tall, REACH), pl.ds(tall + 2 * EDGE - REACH, REACH)
    pad[:, below, :wide] = rows_in[0]
    pad[:, above, :wide] = rows_in[1]
    for k in range(5):
        pad[k, :tall, wide:] = jnp.where(
            lane < LANE // 2,
            pltpu.roll(beside, LANE - 16 - 2 * k, 1),
            pltpu.roll(beside, LANE - 2 - 2 * k, 1),
        )
        pad[k, below, wide:] = jnp.where(near, corner[0, k], corner[1, k])
        pad[k, above, wide:] = jnp.where(near, corner[2, k], corner[3, k])

    @pl.when(at_edge)
    def _():
        pad[3:5, tall:tall + 1, :] = jnp.ones((2, 1, wide + LANE), F32)

    def first_step():
        face = faces(pad[3], pad[4])
        for k in range(4):
            face_buf[k] = face[k]
        new = step_once(pad[0], pad[1], pad[2], pad[3], pad[4], face)
        for k in range(3):
            mid[k] = new[k]

    def second_step():
        face = [face_buf[k] for k in range(4)]
        new = step_once(mid[0], mid[1], mid[2], pad[3], pad[4], face)
        for k in range(3):
            out_buf[k] = new[k][:tall, :wide]

    first_step()

    inputs[8].wait()
    span = wide + LANE

    @pl.when(at_edge)
    def _():
        place = lax.broadcasted_iota(jnp.int32, (span, obs), 0)
        place = jnp.where(place >= wide + LANE // 2, place - span, place) + col * wide
        chosen_buf[...] = jnp.where(place == cells[...], 1.0, 0.0).astype(BF16)

    second_step()

    @pl.when(home)
    def _():
        whole_wait(whole_in.at[pl.ds(0, 2 * depth - 1)], recv_sem.at[3]).wait_recv()

    @pl.when(jnp.logical_not(home))
    def _():
        whole_wait(whole_in, recv_sem.at[3]).wait_recv()

    for half in range(2):
        value = whole_in[half * depth]
        for k in range(1, depth):
            value = value + whole_in[half * depth + k]
        series_buf[:, half * LANE:(half + 1) * LANE] = value

    @pl.when(at_edge)
    def _():
        whole_wait(edge_in.at[pl.ds(0, depth * blocks - 1)], recv_sem.at[2]).wait_recv()
        total = edge_in[pl.ds(0, blocks)]
        for k in range(1, depth):
            total = total + edge_in[pl.ds(k * blocks, blocks)]
        latest = jnp.concatenate([total[b] for b in range(blocks)], axis=1)
        high, rest = split(latest)
        middle, rest = split(rest)
        parts = jnp.concatenate([high.astype(F32), middle.astype(F32), rest, rest], axis=0)
        picked = lax.dot_general(
            parts.astype(BF16), chosen_buf[...], (((1,), (1,)), ((), ())),
            preferred_element_type=F32,
        )
        picked = picked[0:2] + picked[2:4] + picked[4:6]
        base = tall - 2 * EDGE
        part_rows = pl.ds(base, 3 * EDGE)
        at_ghost = lax.broadcasted_iota(jnp.int32, (3 * EDGE, span), 0) == 2 * EDGE
        ghosts = [
            jnp.broadcast_to(picked[k:k + 1], (3 * EDGE, span)) for k in range(2)
        ]
        wet, speed_sq = pad[4, part_rows], pad[3, part_rows]
        face = [face_buf[k, part_rows] for k in range(4)]
        surf = jnp.where(at_ghost, ghosts[0], pad[0, part_rows])
        surf, qx, qy = step_once(
            surf, pad[1, part_rows], pad[2, part_rows], speed_sq, wet, face
        )
        surf = jnp.where(at_ghost, ghosts[1], surf)
        qx = jnp.where(at_ghost, 0.0, qx)
        qy = jnp.where(at_ghost, 0.0, qy)
        new = step_once(surf, qx, qy, speed_sq, wet, face)
        for k in range(3):
            out_buf[k, tall - EDGE:] = new[k][EDGE:2 * EDGE, :wide]

    for exists, _, copy in moves:
        @pl.when(exists)
        def _(copy=copy):
            copy.wait_send()
    for ref, sem in (
        (core_in, send_sem.at[0]), (late_in, send_sem.at[1]),
        (others, send_sem.at[2]),
    ):
        whole_wait(ref, sem).wait_send()

    @pl.when(at_edge)
    def _():
        whole_wait(edge_in.at[pl.ds(0, n_cols - 1)], send_sem.at[3]).wait_send()

    @pl.when(jnp.logical_not(at_edge))
    def _():
        whole_wait(edge_in.at[pl.ds(0, n_cols)], send_sem.at[3]).wait_send()

    @pl.when(home)
    def _():
        whole_wait(whole_in.at[pl.ds(0, 2 * depth - 1)], send_sem.at[4]).wait_send()

    @pl.when(jnp.logical_not(home))
    def _():
        whole_wait(whole_in, send_sem.at[4]).wait_send()


def write_out(series, fields, series_hbm, surf_hbm, qx_hbm, qy_hbm, sems):
    copies = [pltpu.make_async_copy(series, series_hbm, sems.at[3])]
    for k, target in enumerate((surf_hbm, qx_hbm, qy_hbm)):
        copies.append(pltpu.make_async_copy(fields.at[k], target, sems.at[k]))
    for copy in copies:
        copy.start()
    for copy in copies:
        copy.wait()


def on_device(n_rows, n_cols, kernel_hat, coefficients, wave_speed_sq, wet_mask, boundary_cell, height, flux_x, flux_y):
    _, freqs, src, obs = kernel_hat.shape
    steps = coefficients.shape[0]
    tall, wide = height.shape
    points = obs // n_cols
    own_steps = steps // n_rows
    span = wide + LANE
    forward, inverse = tables(freqs * n_rows, steps, n_rows)
    dma = pltpu.SemaphoreType.DMA
    anywhere = pl.BlockSpec(memory_space=pltpu.HBM)
    in_vmem = pl.BlockSpec(memory_space=pltpu.VMEM)
    series, fields = pl.pallas_call(
        functools.partial(kernel, n_rows, n_cols),
        out_shape=(
            pltpu.VMEM((own_steps, points), F32),
            pltpu.VMEM((3, tall, wide), F32),
        ),
        in_specs=[anywhere] * 10,
        out_specs=(in_vmem,) * 2,
        scratch_shapes=[
            pltpu.VMEM((Y, 2, freqs, src, obs // Y), BF16),
            pltpu.VMEM((src, steps), F32),
            pltpu.VMEM(forward.shape[1:], F32),
            pltpu.VMEM(inverse.shape[1:], BF16),
            pltpu.VMEM((1, obs), jnp.int32),
            pltpu.VMEM((5, tall + 2 * EDGE, span), F32),
            pltpu.VMEM((tall, wide), jnp.int32),
            pltpu.VMEM((4, 5, REACH, LANE), F32),
            pltpu.VMEM((2, 5, REACH, wide), F32),
            pltpu.VMEM((2, 5, REACH, wide), F32),
            pltpu.VMEM((32, tall), F32),
            pltpu.VMEM((32, tall), F32),
            pltpu.VMEM((Y, CORES, X, 2 * freqs, LANE), F32),
            pltpu.VMEM((Y, X, 2 * freqs, LANE), F32),
            pltpu.VMEM((Y, X, 2 * freqs, LANE), F32),
            pltpu.VMEM((Y * X, 2 * freqs, LANE), F32),
            pltpu.VMEM((X, 2 * freqs, LANE), F32),
            pltpu.VMEM((steps, LANE), F32),
            pltpu.VMEM((2 * Z_LOW * Z_HIGH, own_steps, LANE), F32),
            pltpu.VMEM((Y, CORES, X, 2, LANE), F32),
            pltpu.VMEM((Y * X * CORES - 1, 2, LANE), F32),
            pltpu.VMEM((2, LANE), F32),
            pltpu.VMEM((Z_LOW * Z_HIGH * (obs // LANE), 2, LANE), F32),
            pltpu.VMEM((4, tall + 2 * EDGE, span), F32),
            pltpu.VMEM((3, tall + 2 * EDGE, span), F32),
            pltpu.VMEM((span, obs), BF16),
            dma((9,)),
            dma((Y, 2)),
            dma((Y,)),
            dma((8,)),
            dma((8,)),
            dma((5,)),
            dma((4,)),
            pltpu.SemaphoreType.REGULAR,
            pltpu.SemaphoreType.REGULAR,
        ],
        compiler_params=pltpu.CompilerParams(
            collective_id=0, has_side_effects=True, vmem_limit_bytes=60 * 1024 * 1024
        ),
    )(
        kernel_hat, coefficients.T, wave_speed_sq, wet_mask, boundary_cell.reshape(1, obs),
        height, flux_x, flux_y, jnp.asarray(forward), jnp.asarray(inverse),
    )
    return pl.pallas_call(
        write_out,
        out_shape=(
            jax.ShapeDtypeStruct((own_steps, points), F32),
            jax.ShapeDtypeStruct((tall, wide), F32),
            jax.ShapeDtypeStruct((tall, wide), F32),
            jax.ShapeDtypeStruct((tall, wide), F32),
        ),
        in_specs=[in_vmem] * 2,
        out_specs=(anywhere,) * 4,
        scratch_shapes=[dma((4,))],
        compiler_params=pltpu.CompilerParams(vmem_limit_bytes=4 * 1024 * 1024),
    )(series, fields)


def solution(mesh):
    n_rows, n_cols = mesh.shape["rows"], mesh.shape["cols"]
    return jax.shard_map(
        functools.partial(on_device, n_rows, n_cols),
        mesh=mesh,
        in_specs=(
            P(None, "rows", "cols", None),
            P(None, "cols"),
            P("rows", "cols"),
            P("rows", "cols"),
            P(),
            P("rows", "cols"),
            P("rows", "cols"),
            P("rows", "cols"),
        ),
        out_specs=(P("rows", "cols"), P("rows", "cols"), P("rows", "cols"), P("rows", "cols")),
        check_vma=False,
    )
```

```python
import functools
import math

import jax
import jax.numpy as jnp
import numpy as np
from jax import lax
from jax.experimental import pallas as pl
from jax.experimental.pallas import tpu as pltpu
from jax.sharding import PartitionSpec as P

MESH = pl.DeviceIdType.MESH
GROUP = 8
LANE = 128
REACH = 2
SHIFT = LANE // 2 + REACH
X, Y, Z_LOW, Z_HIGH, CORES = 4, 4, 4, 2, 2
Y_ORDER = (2, 1, 3, 0)
BARRIER_AFTER = 1
EDGE = 8
F32 = jnp.float32
BF16 = jnp.bfloat16


def halves(table):
    high = table.astype(np.float32).astype(jnp.bfloat16)
    low = (table - high.astype(np.float64)).astype(np.float32).astype(jnp.bfloat16)
    return np.concatenate([high, high, low], axis=2)


def tables(freq_total, steps, row_devs):
    freq = np.arange(freq_total)
    time = np.arange(steps)
    phase = 2.0 * math.pi * (np.outer(freq, time) % freq_total) / freq_total
    cos = np.cos(phase).reshape(row_devs, -1, GROUP, steps)
    sin = np.sin(phase).reshape(row_devs, -1, GROUP, steps)
    both = np.concatenate([cos, -sin], axis=2).reshape(row_devs, -1, steps)
    forward = both.astype(np.float32)
    inverse = np.swapaxes(both, 1, 2) / freq_total
    four = np.swapaxes(both.reshape(row_devs // X, -1, steps), 1, 2) / freq_total
    late = halves(inverse[:, steps - 2 * GROUP:]).astype(np.float32)
    late = np.pad(late, ((0, 0), (0, 0), (0, steps - late.shape[2])))
    return np.concatenate([forward, late], axis=1), halves(four)


def split(value):
    high = value.astype(BF16)
    return high, value - high.astype(F32)


def faces(speed_sq, wet):
    speed = 0.0625 * jnp.sqrt(speed_sq)
    found = []
    for dim in (1, 0):
        ahead = wet.shape[dim] - 1
        opened = wet * pltpu.roll(wet, ahead, dim)
        found += [0.125 * opened, opened * (speed + pltpu.roll(speed, ahead, dim))]
    return found


def step_once(surf, qx, qy, speed_sq, wet, face):
    energy = speed_sq * surf
    change = []
    for dim, along, across, half, damp in ((1, qx, qy, *face[:2]), (0, qy, qx, *face[2:])):
        ahead = surf.shape[dim] - 1
        later = lambda v: pltpu.roll(v, ahead, dim)
        along_later = later(along)
        mass = half * (along + along_later) + damp * (surf - later(surf))
        momentum = half * (energy + later(energy)) + damp * (along - along_later)
        shear = damp * (across - later(across))
        change.append([f - pltpu.roll(f, 1, dim) for f in (mass, momentum, shear)])
    (mass_x, mom_x, shear_x), (mass_y, mom_y, shear_y) = change
    return (
        wet * (surf - (mass_x + mass_y)),
        wet * (qx - (mom_x + shear_y)),
        wet * (qy - (shear_x + mom_y)),
    )


def kernel(
    n_rows, n_cols,
    kern_hbm, coef_hbm, sq_hbm, wet_hbm, cell_hbm, surf_hbm, qx_hbm, qy_hbm, fwd_hbm, inv_hbm,
    series_buf, out_buf,
    kern, coef, fwd, inv, cells, pad, wet_int, corner, rows_out, rows_in, strip_out, strip_in,
    part, core_in, plane_out, plane_in, spec_buf, whole_buf, whole_in,
    late_part, late_in, late_out, edge_in, face_buf, mid, chosen_buf,
    local_sem, kern_sem, core_recv, halo_send, halo_recv, send_sem, recv_sem, near_sem, far_sem,
):
    row = lax.axis_index("rows")
    col = lax.axis_index("cols")
    x, z_low = lax.rem(row, X), row // X
    y, z_high, core = col // (Z_HIGH * CORES), lax.rem(col // CORES, Z_HIGH), lax.rem(col, CORES)
    z = z_high * Z_LOW + z_low
    freqs, src = kern.shape[2:4]
    groups = freqs // GROUP
    tall, wide = surf_hbm.shape
    obs = cells.shape[1]
    points = obs // n_cols
    per_y = obs // Y
    own_steps = series_buf.shape[0]
    has_n, has_s = row > 0, row < n_rows - 1
    has_w, has_e = col > 0, col < n_cols - 1
    at_edge = row == n_rows - 1

    inputs = [
        pltpu.make_async_copy(coef_hbm, coef, local_sem.at[0]),
        pltpu.make_async_copy(fwd_hbm.at[row], fwd, local_sem.at[1]),
        pltpu.make_async_copy(surf_hbm, pad.at[0, :tall, :wide], local_sem.at[3]),
        pltpu.make_async_copy(qx_hbm, pad.at[1, :tall, :wide], local_sem.at[4]),
        pltpu.make_async_copy(qy_hbm, pad.at[2, :tall, :wide], local_sem.at[5]),
        pltpu.make_async_copy(sq_hbm, pad.at[3, :tall, :wide], local_sem.at[6]),
        pltpu.make_async_copy(wet_hbm, wet_int, local_sem.at[7]),
        pltpu.make_async_copy(inv_hbm.at[z_low], inv, local_sem.at[2]),
        pltpu.make_async_copy(cell_hbm, cells, local_sem.at[8]),
    ]
    for copy in inputs[:2]:
        copy.start()
    chunks = []
    for i, dy in enumerate(Y_ORDER):
        at = pl.multiple_of(lax.rem(y + dy, Y) * per_y, per_y)
        for p in range(2):
            copy = pltpu.make_async_copy(
                kern_hbm.at[p, :, :, pl.ds(at, per_y)], kern.at[i, p], kern_sem.at[i, p]
            )
            chunks.append(copy)
    for copy in chunks[:2]:
        copy.start()
    pad[:, tall:] = jnp.zeros((5, 2 * EDGE, wide + LANE), F32)
    rows_in[...] = jnp.zeros(rows_in.shape, F32)
    strip_in[...] = jnp.zeros(strip_in.shape, F32)
    corner[...] = jnp.zeros(corner.shape, F32)

    diagonals = [
        (has_n & has_w, -1, -1), (has_n & has_e, -1, 1),
        (has_s & has_w, 1, -1), (has_s & has_e, 1, 1),
    ]
    plane = [
        (dy, dx, dc) for dy in range(Y) for dx in range(X) for dc in range(CORES) if dy or dx or dc
    ]
    depth = Z_LOW * Z_HIGH
    home = x // Z_HIGH == z_high
    barrier = pltpu.get_barrier_semaphore()

    def greet(to):
        pl.semaphore_signal(barrier, 1, device_id=to, device_id_type=MESH)

    def device(x_at, y_at, z_at, core_at):
        return (
            lax.rem(z_at, Z_LOW) * X + x_at,
            (y_at * Z_HIGH + z_at // Z_LOW) * CORES + core_at,
        )

    def in_plane(dy, dx, dc):
        return device(lax.rem(x + dx, X), lax.rem(y + dy, Y), z, lax.rem(core + dc, CORES))

    partner_core = device(x, y, z, 1 - core)

    def in_line(dz):
        return device(x, y, lax.rem(z + dz + depth, depth), core)

    for dz in (2, -2, 1, -1):
        greet(in_line(dz))
    for copy in chunks[2:4]:
        copy.start()
    for dy, dx, dc in plane:
        greet(in_plane(dy, dx, dc))
    for copy in chunks[4:]:
        copy.start()
    for copy in inputs[2:]:
        copy.start()

    def remote(source, target, send, recv, to):
        return pltpu.make_async_remote_copy(
            src_ref=source, dst_ref=target, send_sem=send, recv_sem=recv,
            device_id=to, device_id_type=MESH,
        )

    def whole_wait(ref, sem):
        return remote(ref, ref, sem, sem, partner_core)

    inputs[0].wait()
    inputs[1].wait()
    spectrum = lax.dot_general(
        fwd[:2 * freqs], coef[...], (((1,), (1,)), ((), ())),
        precision=lax.Precision.HIGHEST, preferred_element_type=F32,
    )
    spread = jnp.where(
        lax.rem(lax.broadcasted_iota(jnp.int32, (src, GROUP * src), 1), src)
        == lax.broadcasted_iota(jnp.int32, (src, GROUP * src), 0), 1.0, 0.0
    ).astype(BF16)
    shape = (2 * GROUP, GROUP * src)
    own_block = (
        lax.broadcasted_iota(jnp.int32, shape, 1) // src
        == lax.rem(lax.broadcasted_iota(jnp.int32, shape, 0), GROUP)
    )
    lefts = []
    for g in range(groups):
        mine = spectrum[g * 2 * GROUP:(g + 1) * 2 * GROUP]
        turned = jnp.concatenate([-mine[GROUP:], mine[:GROUP]], axis=0)
        for value in (mine, turned):
            tiled = jnp.dot(value.astype(BF16), spread, preferred_element_type=F32)
            lefts.append(jnp.where(own_block, tiled, 0.0).astype(BF16))

    def send_chunk(i):
        remote(
            part.at[i, 1 - core], core_in.at[i], send_sem.at[0], core_recv.at[i], partner_core
        ).start()
        for k, (dy, dx, dc) in enumerate(plane):
            if dy == Y_ORDER[i]:
                remote(
                    late_part.at[i, lax.rem(core + dc, CORES), lax.rem(x + dx, X)], late_in.at[k],
                    send_sem.at[1], recv_sem.at[0], in_plane(dy, dx, dc),
                ).start()

    def gather(i):
        whole_wait(core_in.at[i], core_recv.at[i]).wait_recv()
        plane_out[i] = part[i, core] + core_in[i]
        for dx in (2, 1, 3, 0):
            if Y_ORDER[i] or dx:
                remote(
                    plane_out.at[i, lax.rem(x + dx, X)], plane_in.at[(i + 1) % Y * X + dx],
                    send_sem.at[2], recv_sem.at[1], in_plane(Y_ORDER[i], dx, 0),
                ).start()

    tail = fwd[2 * freqs:].astype(BF16)[:, :6 * freqs]
    for i in range(Y):
        chunks[2 * i].wait()
        chunks[2 * i + 1].wait()
        totals = []
        for g in range(groups):
            total = None
            for p in range(2):
                right = kern[i, p, pl.ds(g * GROUP, GROUP)].reshape(GROUP * src, per_y)
                term = jnp.dot(lefts[2 * g + p], right, preferred_element_type=F32)
                total = term if total is None else total + term
            totals.append(total)
        total = jnp.concatenate(totals, axis=0)
        high, low = split(total)
        late = jnp.dot(
            tail, jnp.concatenate([high, low.astype(BF16), high], axis=0),
            preferred_element_type=F32,
        )[2 * GROUP - 2:]
        for h in range(Z_HIGH):
            for c in range(CORES):
                for half in range(2):
                    at = (h * CORES + c) * points + half * LANE
                    part[i, c, 2 * h + half] = total[:, at:at + LANE]
                    late_part[i, c, 2 * h + half] = late[:, at:at + LANE]
        if i == BARRIER_AFTER:
            pl.semaphore_wait(barrier, len(plane) + 4)
            for dz in (2, -2, 1, -1):
                pl.semaphore_signal(
                    near_sem, 1, device_id=in_line(dz), device_id_type=MESH
                )
            for j in range(i + 1):
                send_chunk(j)
        elif i > BARRIER_AFTER:
            send_chunk(i)
        if i == Y - 2:
            gather(0)

    gather(1)
    for copy in inputs[2:7]:
        copy.wait()
    pad[4, :tall, :wide] = wet_int[...].astype(F32)
    lane = lax.broadcasted_iota(jnp.int32, (tall, LANE), 1)
    packed = jnp.zeros((tall, LANE), F32)
    for k in range(5):
        first, last = pad[k, :tall, :LANE], pad[k, :tall, wide - LANE:wide]
        at = 2 * k
        moved = first if at == 0 else pltpu.roll(first, at, 1)
        packed = jnp.where((lane >= at) & (lane < at + 2), moved, packed)
        at = 16 + 2 * k
        packed = jnp.where(
            (lane >= at) & (lane < at + 2), pltpu.roll(last, at + 2, 1), packed
        )
    strip_out[...] = packed.T[:32]
    rows_out[0] = pad[:, :REACH, :wide]
    rows_out[1] = pad[:, tall - REACH:tall, :wide]

    gather(2)

    north = (lax.rem(row + n_rows - 1, n_rows), col)
    south = (lax.rem(row + 1, n_rows), col)
    west = (row, lax.rem(col + n_cols - 1, n_cols))
    east = (row, lax.rem(col + 1, n_cols))
    def halo(source, target, i, to):
        return remote(source, target, halo_send.at[i], halo_recv.at[i], to)

    moves = [
        (has_n, has_s, halo(rows_out.at[0], rows_in.at[0], 0, north), True),
        (has_s, has_n, halo(rows_out.at[1], rows_in.at[1], 1, south), True),
        (has_w, has_e, halo(strip_out.at[pl.ds(0, 16)], strip_in.at[pl.ds(16, 16)], 2, west), core == 1),
        (has_e, has_w, halo(strip_out.at[pl.ds(16, 16)], strip_in.at[pl.ds(0, 16)], 3, east), core == 0),
    ]
    for i, (exists, dr, dc) in enumerate(diagonals):
        side = 0 if dr < 0 else 1
        cols_at = pl.ds(0, LANE) if dc < 0 else pl.ds(wide - LANE, LANE)
        to = (lax.rem(row + dr + n_rows, n_rows), lax.rem(col + dc + n_cols, n_cols))
        moves.append((
            exists, diagonals[3 - i][0],
            halo(rows_out.at[side, :, :, cols_at], corner.at[i], 4 + i, to),
            core == (1 if dc < 0 else 0),
        ))

    def send_halos(near_ones):
        for exists, _, copy, near in moves:
            if near is True:
                if near_ones:
                    pl.when(exists)(copy.start)
            else:
                pl.when(exists & (near if near_ones else jnp.logical_not(near)))(copy.start)

    pl.semaphore_wait(near_sem, 4)
    for dz in (2, -2):
        pl.semaphore_signal(far_sem, 1, device_id=in_line(dz), device_id_type=MESH)
    send_halos(True)
    gather(Y - 1)
    pl.semaphore_wait(far_sem, 2)
    send_halos(False)

    whole_wait(late_in, recv_sem.at[0]).wait_recv()
    late = late_part[Y - 1, core, x]
    for k in range(len(plane)):
        late = late + late_in[k]
    late_out[...] = late
    block = ((y * Z_HIGH + x // 2) * CORES + core) * 2 + lax.rem(x, 2)
    blocks = obs // LANE
    for k in range(n_cols):
        def _(k=k):
            remote(
                late_out, edge_in.at[z * blocks + block], send_sem.at[3], recv_sem.at[2],
                (n_rows - 1, lax.rem(col + k, n_cols)),
            ).start()
        if k:
            _()
        else:
            pl.when(jnp.logical_not(at_edge))(_)

    @pl.when(at_edge)
    def _():
        edge_in[z * blocks + block] = late

    others = plane_in.at[pl.ds(1, X * Y - 1)]
    whole_wait(others, recv_sem.at[1]).wait_recv()
    for dx in range(X):
        value = plane_out[Y - 1, x] if dx == 0 else plane_in[dx]
        for i in range(Y - 1):
            value = value + plane_in[(i + 1) * X + dx]
        spec_buf[lax.rem(x + X - dx, X)] = value
    inputs[7].wait()
    high, low = split(spec_buf[...].reshape(X * 2 * freqs, LANE))
    whole = jnp.dot(
        inv[...], jnp.concatenate([high, low.astype(BF16), high], axis=0),
        preferred_element_type=F32,
    )
    whole_buf[...] = whole
    z_base = x // 2 * Z_LOW
    own_half = lax.rem(x, 2) * depth
    for k in range(n_rows):
        def _(k=k):
            to = lax.rem(row + k, n_rows)
            z_to = z_base + to // X
            remote(
                whole_buf.at[pl.ds(pl.multiple_of(to * own_steps, own_steps), own_steps)],
                whole_in.at[own_half + lax.rem(z_to - z + depth, depth)],
                send_sem.at[4], recv_sem.at[3], device(lax.rem(to, X), y, z_to, core),
            ).start()
        if k:
            _()
        else:
            pl.when(jnp.logical_not(home))(_)

    @pl.when(home)
    def _():
        whole_in[own_half] = whole_buf[
            pl.ds(pl.multiple_of(row * own_steps, own_steps), own_steps)
        ]

    def arrive(some):
        for _, arrives, copy, _ in some:
            @pl.when(arrives)
            def _(copy=copy):
                copy.wait_recv()

    arrive(moves[:2])
    span = wide + LANE
    below, above = pl.ds(tall, REACH), pl.ds(tall + 2 * EDGE - REACH, REACH)
    pad[:, below, :wide] = rows_in[0]
    pad[:, above, :wide] = rows_in[1]

    @pl.when(at_edge)
    def _():
        pad[3:5, tall:tall + 1, :wide] = jnp.ones((2, 1, wide), F32)

    def first_step(lanes):
        face = faces(pad[3, :, lanes], pad[4, :, lanes])
        for k in range(4):
            face_buf[k, :, lanes] = face[k]
        new = step_once(*(pad[k, :, lanes] for k in range(5)), face)
        for k in range(3):
            mid[k, :, lanes] = new[k]

    def second_step(lanes):
        face = [face_buf[k, :, lanes] for k in range(4)]
        state = [mid[k, :, lanes] for k in range(3)]
        return step_once(*state, pad[3, :, lanes], pad[4, :, lanes], face)

    def place_sides(k, rows, sides):
        at = lax.broadcasted_iota(jnp.int32, sides.shape, 1)
        first, last = pl.ds(0, LANE), pl.ds(wide - LANE, LANE)
        out_buf[k, rows, first] = jnp.where(
            at < REACH, pltpu.roll(sides, LANE - SHIFT, 1), out_buf[k, rows, first]
        )
        out_buf[k, rows, last] = jnp.where(
            at >= LANE - REACH, pltpu.roll(sides, SHIFT, 1), out_buf[k, rows, last]
        )

    body, border = pl.ds(0, wide), pl.ds(wide, LANE)
    first_step(body)
    new = second_step(body)
    for k in range(3):
        out_buf[k] = new[k][:tall]
    left = lax.broadcasted_iota(jnp.int32, (tall + 2 * EDGE, LANE), 1) < LANE // 2
    for k in range(5):
        pad[k, :, border] = jnp.where(
            left,
            pltpu.roll(pad[k, :, wide - LANE:wide], LANE - SHIFT, 1),
            pltpu.roll(pad[k, :, :LANE], SHIFT, 1),
        )

    arrive(moves[2:])
    beside = jnp.concatenate([strip_in[...], jnp.zeros((LANE - 32, tall), F32)], axis=0).T
    edge_at = LANE // 2 - REACH

    def lay(k, rows, from_west, from_east):
        at = lax.broadcasted_iota(jnp.int32, from_west.shape, 1)
        value = jnp.where(at < LANE // 2, from_east, from_west)
        pad[k, rows, border] = jnp.where(
            (at >= edge_at) & (at < edge_at + 2 * REACH), value, pad[k, rows, border]
        )

    for k in range(5):
        lay(
            k, pl.ds(0, tall), pltpu.roll(beside, LANE // 2 - 2 * k, 1),
            pltpu.roll(beside, edge_at - 16 - 2 * k, 1),
        )
        for i, rows in ((0, below), (2, above)):
            lay(
                k, rows, pltpu.roll(corner[i + 1, k], SHIFT, 1),
                pltpu.roll(corner[i, k], edge_at, 1),
            )

    @pl.when(at_edge)
    def _():
        pad[3:5, tall:tall + 1, wide:] = jnp.ones((2, 1, LANE), F32)

    first_step(border)
    new = second_step(border)
    for k in range(3):
        place_sides(k, pl.ds(0, tall), new[k][:tall])

    inputs[8].wait()

    @pl.when(at_edge)
    def _():
        place = lax.broadcasted_iota(jnp.int32, (span, obs), 0)
        place = col * wide + place - jnp.where(
            place >= wide + LANE // 2, wide + SHIFT, jnp.where(place >= wide, SHIFT - REACH - REACH, 0)
        )
        chosen_buf[...] = jnp.where(place == cells[...], 1.0, 0.0).astype(BF16)

    @pl.when(home)
    def _():
        whole_wait(whole_in.at[pl.ds(0, 2 * depth - 1)], recv_sem.at[3]).wait_recv()

    @pl.when(jnp.logical_not(home))
    def _():
        whole_wait(whole_in, recv_sem.at[3]).wait_recv()

    for half in range(2):
        value = whole_in[half * depth]
        for k in range(1, depth):
            value = value + whole_in[half * depth + k]
        series_buf[:, half * LANE:(half + 1) * LANE] = value

    @pl.when(at_edge)
    def _():
        whole_wait(edge_in.at[pl.ds(0, depth * blocks - 1)], recv_sem.at[2]).wait_recv()
        total = edge_in[pl.ds(0, blocks)]
        for k in range(1, depth):
            total = total + edge_in[pl.ds(k * blocks, blocks)]
        latest = jnp.concatenate([total[b] for b in range(blocks)], axis=1)
        high, rest = split(latest)
        middle, rest = split(rest)
        parts = jnp.concatenate([high.astype(F32), middle.astype(F32), rest, rest], axis=0)
        picked = lax.dot_general(
            parts.astype(BF16), chosen_buf[...], (((1,), (1,)), ((), ())),
            preferred_element_type=F32,
        )
        picked = picked[0:2] + picked[2:4] + picked[4:6]
        base = tall - 2 * EDGE
        part_rows = pl.ds(base, 3 * EDGE)
        for lanes in (body, border):
            width = lanes.size
            picks = picked[:, lanes.start:lanes.start + width]
            at_ghost = lax.broadcasted_iota(jnp.int32, (3 * EDGE, width), 0) == 2 * EDGE
            ghosts = [jnp.broadcast_to(picks[k:k + 1], (3 * EDGE, width)) for k in range(2)]
            speed_sq, wet = pad[3, part_rows, lanes], pad[4, part_rows, lanes]
            face = [face_buf[k, part_rows, lanes] for k in range(4)]
            surf = jnp.where(at_ghost, ghosts[0], pad[0, part_rows, lanes])
            surf, qx, qy = step_once(
                surf, pad[1, part_rows, lanes], pad[2, part_rows, lanes], speed_sq, wet, face
            )
            surf = jnp.where(at_ghost, ghosts[1], surf)
            qx = jnp.where(at_ghost, 0.0, qx)
            qy = jnp.where(at_ghost, 0.0, qy)
            new = step_once(surf, qx, qy, speed_sq, wet, face)
            for k in range(3):
                if width == wide:
                    out_buf[k, tall - EDGE:] = new[k][EDGE:2 * EDGE]
                else:
                    place_sides(k, pl.ds(tall - EDGE, EDGE), new[k][EDGE:2 * EDGE])

    for exists, _, copy, _ in moves:
        @pl.when(exists)
        def _(copy=copy):
            copy.wait_send()
    for ref, sem in (
        (core_in, send_sem.at[0]), (late_in, send_sem.at[1]),
        (others, send_sem.at[2]),
    ):
        whole_wait(ref, sem).wait_send()

    @pl.when(at_edge)
    def _():
        whole_wait(edge_in.at[pl.ds(0, n_cols - 1)], send_sem.at[3]).wait_send()

    @pl.when(jnp.logical_not(at_edge))
    def _():
        whole_wait(edge_in.at[pl.ds(0, n_cols)], send_sem.at[3]).wait_send()

    @pl.when(home)
    def _():
        whole_wait(whole_in.at[pl.ds(0, 2 * depth - 1)], send_sem.at[4]).wait_send()

    @pl.when(jnp.logical_not(home))
    def _():
        whole_wait(whole_in, send_sem.at[4]).wait_send()


def write_out(series, fields, series_hbm, surf_hbm, qx_hbm, qy_hbm, sems):
    copies = [pltpu.make_async_copy(series, series_hbm, sems.at[3])]
    for k, target in enumerate((surf_hbm, qx_hbm, qy_hbm)):
        copies.append(pltpu.make_async_copy(fields.at[k], target, sems.at[k]))
    for copy in copies:
        copy.start()
    for copy in copies:
        copy.wait()


def on_device(n_rows, n_cols, kernel_hat, coefficients, wave_speed_sq, wet_mask, boundary_cell, height, flux_x, flux_y):
    _, freqs, src, obs = kernel_hat.shape
    steps = coefficients.shape[0]
    tall, wide = height.shape
    points = obs // n_cols
    own_steps = steps // n_rows
    span = wide + LANE
    forward, inverse = tables(freqs * n_rows, steps, n_rows)
    dma = pltpu.SemaphoreType.DMA
    anywhere = pl.BlockSpec(memory_space=pltpu.HBM)
    in_vmem = pl.BlockSpec(memory_space=pltpu.VMEM)
    series, fields = pl.pallas_call(
        functools.partial(kernel, n_rows, n_cols),
        out_shape=(
            pltpu.VMEM((own_steps, points), F32),
            pltpu.VMEM((3, tall, wide), F32),
        ),
        in_specs=[anywhere] * 10,
        out_specs=(in_vmem,) * 2,
        scratch_shapes=[
            pltpu.VMEM((Y, 2, freqs, src, obs // Y), BF16),
            pltpu.VMEM((src, steps), F32),
            pltpu.VMEM(forward.shape[1:], F32),
            pltpu.VMEM(inverse.shape[1:], BF16),
            pltpu.VMEM((1, obs), jnp.int32),
            pltpu.VMEM((5, tall + 2 * EDGE, span), F32),
            pltpu.VMEM((tall, wide), jnp.int32),
            pltpu.VMEM((4, 5, REACH, LANE), F32),
            pltpu.VMEM((2, 5, REACH, wide), F32),
            pltpu.VMEM((2, 5, REACH, wide), F32),
            pltpu.VMEM((32, tall), F32),
            pltpu.VMEM((32, tall), F32),
            pltpu.VMEM((Y, CORES, X, 2 * freqs, LANE), F32),
            pltpu.VMEM((Y, X, 2 * freqs, LANE), F32),
            pltpu.VMEM((Y, X, 2 * freqs, LANE), F32),
            pltpu.VMEM((Y * X, 2 * freqs, LANE), F32),
            pltpu.VMEM((X, 2 * freqs, LANE), F32),
            pltpu.VMEM((steps, LANE), F32),
            pltpu.VMEM((2 * Z_LOW * Z_HIGH, own_steps, LANE), F32),
            pltpu.VMEM((Y, CORES, X, 2, LANE), F32),
            pltpu.VMEM((Y * X * CORES - 1, 2, LANE), F32),
            pltpu.VMEM((2, LANE), F32),
            pltpu.VMEM((Z_LOW * Z_HIGH * (obs // LANE), 2, LANE), F32),
            pltpu.VMEM((4, tall + 2 * EDGE, span), F32),
            pltpu.VMEM((3, tall + 2 * EDGE, span), F32),
            pltpu.VMEM((span, obs), BF16),
            dma((9,)),
            dma((Y, 2)),
            dma((Y,)),
            dma((8,)),
            dma((8,)),
            dma((5,)),
            dma((4,)),
            pltpu.SemaphoreType.REGULAR,
            pltpu.SemaphoreType.REGULAR,
        ],
        compiler_params=pltpu.CompilerParams(
            collective_id=0, has_side_effects=True, vmem_limit_bytes=60 * 1024 * 1024
        ),
    )(
        kernel_hat, coefficients.T, wave_speed_sq, wet_mask, boundary_cell.reshape(1, obs),
        height, flux_x, flux_y, jnp.asarray(forward), jnp.asarray(inverse),
    )
    return pl.pallas_call(
        write_out,
        out_shape=(
            jax.ShapeDtypeStruct((own_steps, points), F32),
            jax.ShapeDtypeStruct((tall, wide), F32),
            jax.ShapeDtypeStruct((tall, wide), F32),
            jax.ShapeDtypeStruct((tall, wide), F32),
        ),
        in_specs=[in_vmem] * 2,
        out_specs=(anywhere,) * 4,
        scratch_shapes=[dma((4,))],
        compiler_params=pltpu.CompilerParams(vmem_limit_bytes=4 * 1024 * 1024),
    )(series, fields)


def solution(mesh):
    n_rows, n_cols = mesh.shape["rows"], mesh.shape["cols"]
    return jax.shard_map(
        functools.partial(on_device, n_rows, n_cols),
        mesh=mesh,
        in_specs=(
            P(None, "rows", "cols", None),
            P(None, "cols"),
            P("rows", "cols"),
            P("rows", "cols"),
            P(),
            P("rows", "cols"),
            P("rows", "cols"),
            P("rows", "cols"),
        ),
        out_specs=(P("rows", "cols"), P("rows", "cols"), P("rows", "cols"), P("rows", "cols")),
        check_vma=False,
    )
```

```python
import functools
import math

import jax
import jax.numpy as jnp
import numpy as np
from jax import lax
from jax.experimental import pallas as pl
from jax.experimental.pallas import tpu as pltpu
from jax.sharding import PartitionSpec as P

MESH = pl.DeviceIdType.MESH
GROUP = 8
LANE = 128
REACH = 2
SHIFT = LANE // 2 + REACH
X, Y, Z_LOW, Z_HIGH, CORES = 4, 4, 4, 2, 2
Y_ORDER = (2, 1, 3, 0)
BARRIER_AFTER = 1
EDGE = 8
F32 = jnp.float32
BF16 = jnp.bfloat16


def halves(table):
    high = table.astype(np.float32).astype(jnp.bfloat16)
    low = (table - high.astype(np.float64)).astype(np.float32).astype(jnp.bfloat16)
    return np.concatenate([high, high, low], axis=2)


def tables(freq_total, steps, row_devs):
    freq = np.arange(freq_total)
    time = np.arange(steps)
    phase = 2.0 * math.pi * (np.outer(freq, time) % freq_total) / freq_total
    cos = np.cos(phase).reshape(row_devs, -1, GROUP, steps)
    sin = np.sin(phase).reshape(row_devs, -1, GROUP, steps)
    both = np.concatenate([cos, -sin], axis=2).reshape(row_devs, -1, steps)
    forward = both.astype(np.float32)
    inverse = np.swapaxes(both, 1, 2) / freq_total
    four = np.swapaxes(both.reshape(row_devs // X, -1, steps), 1, 2) / freq_total
    late = halves(inverse[:, steps - 2 * GROUP:]).astype(np.float32)
    late = np.pad(late, ((0, 0), (0, 0), (0, steps - late.shape[2])))
    return np.concatenate([forward, late], axis=1), halves(four)


def split(value):
    high = value.astype(BF16)
    return high, value - high.astype(F32)


def faces(speed_sq, wet):
    speed = 0.0625 * jnp.sqrt(speed_sq)
    found = []
    for dim in (1, 0):
        ahead = wet.shape[dim] - 1
        opened = wet * pltpu.roll(wet, ahead, dim)
        found += [0.125 * opened, opened * (speed + pltpu.roll(speed, ahead, dim))]
    return found


def step_once(surf, qx, qy, speed_sq, wet, face):
    energy = speed_sq * surf
    change = []
    for dim, along, across, half, damp in ((1, qx, qy, *face[:2]), (0, qy, qx, *face[2:])):
        ahead = surf.shape[dim] - 1
        later = lambda v: pltpu.roll(v, ahead, dim)
        along_later = later(along)
        mass = half * (along + along_later) + damp * (surf - later(surf))
        momentum = half * (energy + later(energy)) + damp * (along - along_later)
        shear = damp * (across - later(across))
        change.append([f - pltpu.roll(f, 1, dim) for f in (mass, momentum, shear)])
    (mass_x, mom_x, shear_x), (mass_y, mom_y, shear_y) = change
    return (
        wet * (surf - (mass_x + mass_y)),
        wet * (qx - (mom_x + shear_y)),
        wet * (qy - (shear_x + mom_y)),
    )


def kernel(
    n_rows, n_cols,
    kern_hbm, coef_hbm, sq_hbm, wet_hbm, cell_hbm, surf_hbm, qx_hbm, qy_hbm, fwd_hbm, inv_hbm,
    series_buf, out_buf,
    kern, coef, fwd, inv, cells, pad, wet_int, corner, rows_out, rows_in, strip_out, strip_in,
    part, core_in, plane_out, plane_in, spec_buf, whole_buf, whole_in,
    late_part, late_in, late_out, edge_in, both_cores, face_buf, mid, chosen_buf,
    local_sem, kern_sem, core_recv, halo_send, halo_recv, recv_sem, near_sem, far_sem,
):
    row = lax.axis_index("rows")
    col = lax.axis_index("cols")
    x, z_low = lax.rem(row, X), row // X
    y, z_high, core = col // (Z_HIGH * CORES), lax.rem(col // CORES, Z_HIGH), lax.rem(col, CORES)
    z = z_high * Z_LOW + z_low
    freqs, src = kern.shape[2:4]
    groups = freqs // GROUP
    tall, wide = surf_hbm.shape
    obs = cells.shape[1]
    points = obs // n_cols
    per_y = obs // Y
    own_steps = series_buf.shape[0]
    has_n, has_s = row > 0, row < n_rows - 1
    has_w, has_e = col > 0, col < n_cols - 1
    at_edge = row == n_rows - 1

    inputs = [
        pltpu.make_async_copy(coef_hbm, coef, local_sem.at[0]),
        pltpu.make_async_copy(fwd_hbm.at[row], fwd, local_sem.at[1]),
        pltpu.make_async_copy(surf_hbm, pad.at[0, :tall, :wide], local_sem.at[3]),
        pltpu.make_async_copy(qx_hbm, pad.at[1, :tall, :wide], local_sem.at[3]),
        pltpu.make_async_copy(qy_hbm, pad.at[2, :tall, :wide], local_sem.at[3]),
        pltpu.make_async_copy(sq_hbm, pad.at[3, :tall, :wide], local_sem.at[3]),
        pltpu.make_async_copy(wet_hbm, wet_int, local_sem.at[3]),
        pltpu.make_async_copy(inv_hbm.at[z_low], inv, local_sem.at[2]),
        pltpu.make_async_copy(cell_hbm, cells, local_sem.at[4]),
    ]
    for copy in inputs[:2]:
        copy.start()
    chunks = []
    for i, dy in enumerate(Y_ORDER):
        at = pl.multiple_of(lax.rem(y + dy, Y) * per_y, per_y)
        chunks.append(pltpu.make_async_copy(
            kern_hbm.at[:, :, :, pl.ds(at, per_y)], kern.at[i], kern_sem.at[i]
        ))
    chunks[0].start()
    pad[:, tall:] = jnp.zeros((5, 2 * EDGE, wide + LANE), F32)
    rows_in[...] = jnp.zeros(rows_in.shape, F32)
    strip_in[...] = jnp.zeros(strip_in.shape, F32)
    corner[...] = jnp.zeros(corner.shape, F32)

    diagonals = [
        (has_n & has_w, -1, -1), (has_n & has_e, -1, 1),
        (has_s & has_w, 1, -1), (has_s & has_e, 1, 1),
    ]
    plane = [
        (dy, dx, dc) for dy in range(Y) for dx in range(X) for dc in range(CORES) if dy or dx or dc
    ]
    depth = Z_LOW * Z_HIGH
    home = x // Z_HIGH == z_high
    barrier = pltpu.get_barrier_semaphore()

    def greet(to):
        pl.semaphore_signal(barrier, 1, device_id=to, device_id_type=MESH)

    def device(x_at, y_at, z_at, core_at):
        return (
            lax.rem(z_at, Z_LOW) * X + x_at,
            (y_at * Z_HIGH + z_at // Z_LOW) * CORES + core_at,
        )

    def in_plane(dy, dx, dc):
        return device(lax.rem(x + dx, X), lax.rem(y + dy, Y), z, lax.rem(core + dc, CORES))

    partner_core = device(x, y, z, 1 - core)

    def in_line(dz):
        return device(x, y, lax.rem(z + dz + depth, depth), core)

    for dz in (2, -2, 1, -1):
        greet(in_line(dz))
    chunks[1].start()
    for dy, dx, dc in plane:
        greet(in_plane(dy, dx, dc))
    for copy in chunks[2:]:
        copy.start()
    for copy in inputs[2:]:
        copy.start()

    def remote(source, target, send, recv, to):
        return pltpu.make_async_remote_copy(
            src_ref=source, dst_ref=target, send_sem=send, recv_sem=recv,
            device_id=to, device_id_type=MESH,
        )

    def whole_wait(ref, sem):
        return remote(ref, ref, sem, sem, partner_core)

    inputs[0].wait()
    inputs[1].wait()
    spectrum = lax.dot_general(
        fwd[:2 * freqs], coef[...], (((1,), (1,)), ((), ())),
        precision=lax.Precision.HIGHEST, preferred_element_type=F32,
    )
    spread = jnp.where(
        lax.rem(lax.broadcasted_iota(jnp.int32, (src, GROUP * src), 1), src)
        == lax.broadcasted_iota(jnp.int32, (src, GROUP * src), 0), 1.0, 0.0
    ).astype(BF16)
    shape = (2 * GROUP, GROUP * src)
    own_block = (
        lax.broadcasted_iota(jnp.int32, shape, 1) // src
        == lax.rem(lax.broadcasted_iota(jnp.int32, shape, 0), GROUP)
    )
    lefts = []
    for g in range(groups):
        mine = spectrum[g * 2 * GROUP:(g + 1) * 2 * GROUP]
        turned = jnp.concatenate([-mine[GROUP:], mine[:GROUP]], axis=0)
        for value in (mine, turned):
            tiled = jnp.dot(value.astype(BF16), spread, preferred_element_type=F32)
            lefts.append(jnp.where(own_block, tiled, 0.0).astype(BF16))

    def send_chunk(i):
        remote(
            part.at[i, 1 - core], core_in.at[i], local_sem.at[0], core_recv.at[i], partner_core
        ).start()
        for k, (dy, dx, dc) in enumerate(plane):
            if dy == Y_ORDER[i]:
                remote(
                    late_part.at[i, lax.rem(core + dc, CORES), lax.rem(x + dx, X)], late_in.at[k],
                    local_sem.at[1], recv_sem.at[0], in_plane(dy, dx, dc),
                ).start()

    def gather(i):
        whole_wait(core_in.at[i], core_recv.at[i]).wait_recv()
        plane_out[i] = part[i, core] + core_in[i]
        for dx in (2, 1, 3, 0):
            if Y_ORDER[i] or dx:
                remote(
                    plane_out.at[i, lax.rem(x + dx, X)], plane_in.at[(i + 1) % Y * X + dx],
                    kern_sem.at[0], recv_sem.at[1], in_plane(Y_ORDER[i], dx, 0),
                ).start()

    tail = fwd[2 * freqs:].astype(BF16)[:, :6 * freqs]
    for i in range(Y):
        chunks[i].wait()
        totals = []
        for g in range(groups):
            total = None
            for p in range(2):
                right = kern[i, p, pl.ds(g * GROUP, GROUP)].reshape(GROUP * src, per_y)
                term = jnp.dot(lefts[2 * g + p], right, preferred_element_type=F32)
                total = term if total is None else total + term
            totals.append(total)
        total = jnp.concatenate(totals, axis=0)
        high, low = split(total)
        late = jnp.dot(
            tail, jnp.concatenate([high, low.astype(BF16), high], axis=0),
            preferred_element_type=F32,
        )[2 * GROUP - 2:]
        for h in range(Z_HIGH):
            for c in range(CORES):
                for half in range(2):
                    at = (h * CORES + c) * points + half * LANE
                    part[i, c, 2 * h + half] = total[:, at:at + LANE]
                    late_part[i, c, 2 * h + half] = late[:, at:at + LANE]
        if i == BARRIER_AFTER:
            pl.semaphore_wait(barrier, len(plane) + 4)
            for dz in (2, -2, 1, -1):
                pl.semaphore_signal(
                    near_sem, 1, device_id=in_line(dz), device_id_type=MESH
                )
            for j in range(i + 1):
                send_chunk(j)
        elif i > BARRIER_AFTER:
            send_chunk(i)
        if i == Y - 2:
            gather(0)

    gather(1)
    fields = pad.at[:, :tall, :wide]
    pltpu.make_async_copy(fields, fields, local_sem.at[3]).wait()
    pad[4, :tall, :wide] = wet_int[...].astype(F32)
    lane = lax.broadcasted_iota(jnp.int32, (tall, LANE), 1)
    packed = jnp.zeros((tall, LANE), F32)
    for k in range(5):
        first, last = pad[k, :tall, :LANE], pad[k, :tall, wide - LANE:wide]
        at = 2 * k
        moved = first if at == 0 else pltpu.roll(first, at, 1)
        packed = jnp.where((lane >= at) & (lane < at + 2), moved, packed)
        at = 16 + 2 * k
        packed = jnp.where(
            (lane >= at) & (lane < at + 2), pltpu.roll(last, at + 2, 1), packed
        )
    strip_out[...] = packed.T[:32]
    rows_out[0] = pad[:, :REACH, :wide]
    rows_out[1] = pad[:, tall - REACH:tall, :wide]

    gather(2)

    north = (lax.rem(row + n_rows - 1, n_rows), col)
    south = (lax.rem(row + 1, n_rows), col)
    west = (row, lax.rem(col + n_cols - 1, n_cols))
    east = (row, lax.rem(col + 1, n_cols))
    def halo(source, target, i, to):
        return remote(source, target, halo_send.at[i], halo_recv.at[i], to)

    moves = [
        (has_n, has_s, halo(rows_out.at[0], rows_in.at[0], 0, north), True),
        (has_s, has_n, halo(rows_out.at[1], rows_in.at[1], 1, south), True),
        (has_w, has_e, halo(strip_out.at[pl.ds(0, 16)], strip_in.at[pl.ds(16, 16)], 2, west), core == 1),
        (has_e, has_w, halo(strip_out.at[pl.ds(16, 16)], strip_in.at[pl.ds(0, 16)], 3, east), core == 0),
    ]
    for i, (exists, dr, dc) in enumerate(diagonals):
        side = 0 if dr < 0 else 1
        cols_at = pl.ds(0, LANE) if dc < 0 else pl.ds(wide - LANE, LANE)
        to = (lax.rem(row + dr + n_rows, n_rows), lax.rem(col + dc + n_cols, n_cols))
        moves.append((
            exists, diagonals[3 - i][0],
            halo(rows_out.at[side, :, :, cols_at], corner.at[i], 4 + i, to),
            core == (1 if dc < 0 else 0),
        ))

    def send_halos(near_ones):
        for exists, _, copy, near in moves:
            if near is True:
                if near_ones:
                    pl.when(exists)(copy.start)
            else:
                pl.when(exists & (near if near_ones else jnp.logical_not(near)))(copy.start)

    pl.semaphore_wait(near_sem, 4)
    for dz in (2, -2):
        pl.semaphore_signal(far_sem, 1, device_id=in_line(dz), device_id_type=MESH)
    send_halos(True)
    gather(Y - 1)
    pl.semaphore_wait(far_sem, 2)
    send_halos(False)

    whole_wait(late_in, recv_sem.at[0]).wait_recv()
    late = late_part[Y - 1, core, x]
    for k in range(len(plane)):
        late = late + late_in[k]
    late_out[...] = late
    slot = z * (Y * X) + y * X + x
    slots = depth * Y * X
    edges = Y * Z_HIGH
    own_edge = y * Z_HIGH + z_high
    for k in range(edges):
        def _(k=k):
            to = lax.rem(own_edge + k, edges) * CORES + core
            remote(
                late_out, edge_in.at[slot], kern_sem.at[1], recv_sem.at[2], (n_rows - 1, to)
            ).start()
        if k:
            _()
        else:
            pl.when(jnp.logical_not(at_edge))(_)

    @pl.when(at_edge)
    def _():
        edge_in[slot] = late

    others = plane_in.at[pl.ds(1, X * Y - 1)]
    whole_wait(others, recv_sem.at[1]).wait_recv()
    for dx in range(X):
        value = plane_out[Y - 1, x] if dx == 0 else plane_in[dx]
        for i in range(Y - 1):
            value = value + plane_in[(i + 1) * X + dx]
        spec_buf[lax.rem(x + X - dx, X)] = value
    inputs[7].wait()
    high, low = split(spec_buf[...].reshape(X * 2 * freqs, LANE))
    whole = jnp.dot(
        inv[...], jnp.concatenate([high, low.astype(BF16), high], axis=0),
        preferred_element_type=F32,
    )
    whole_buf[...] = whole
    z_base = x // 2 * Z_LOW
    own_half = lax.rem(x, 2) * depth
    for to in range(n_rows):
        @pl.when(jnp.logical_not(home & (row == to)))
        def _(to=to):
            z_to = z_base + to // X
            remote(
                whole_buf.at[pl.ds(to * own_steps, own_steps)],
                whole_in.at[own_half + lax.rem(z_to - z + depth, depth)],
                kern_sem.at[2], recv_sem.at[3], device(to % X, y, z_to, core),
            ).start()

    @pl.when(home)
    def _():
        whole_in[own_half] = whole_buf[
            pl.ds(pl.multiple_of(row * own_steps, own_steps), own_steps)
        ]

    def arrive(some):
        for _, arrives, copy, _ in some:
            @pl.when(arrives)
            def _(copy=copy):
                copy.wait_recv()

    arrive(moves[:2])
    span = wide + LANE
    below, above = pl.ds(tall, REACH), pl.ds(tall + 2 * EDGE - REACH, REACH)
    pad[:, below, :wide] = rows_in[0]
    pad[:, above, :wide] = rows_in[1]

    @pl.when(at_edge)
    def _():
        pad[3:5, tall:tall + 1, :wide] = jnp.ones((2, 1, wide), F32)

    def first_step(lanes):
        face = faces(pad[3, :, lanes], pad[4, :, lanes])
        for k in range(4):
            face_buf[k, :, lanes] = face[k]
        new = step_once(*(pad[k, :, lanes] for k in range(5)), face)
        for k in range(3):
            mid[k, :, lanes] = new[k]

    def second_step(lanes):
        face = [face_buf[k, :, lanes] for k in range(4)]
        state = [mid[k, :, lanes] for k in range(3)]
        return step_once(*state, pad[3, :, lanes], pad[4, :, lanes], face)

    def place_sides(k, rows, sides):
        at = lax.broadcasted_iota(jnp.int32, sides.shape, 1)
        first, last = pl.ds(0, LANE), pl.ds(wide - LANE, LANE)
        out_buf[k, rows, first] = jnp.where(
            at < REACH, pltpu.roll(sides, LANE - SHIFT, 1), out_buf[k, rows, first]
        )
        out_buf[k, rows, last] = jnp.where(
            at >= LANE - REACH, pltpu.roll(sides, SHIFT, 1), out_buf[k, rows, last]
        )

    body, border = pl.ds(0, wide), pl.ds(wide, LANE)
    first_step(body)
    new = second_step(body)
    for k in range(3):
        out_buf[k] = new[k][:tall]
    left = lax.broadcasted_iota(jnp.int32, (tall + 2 * EDGE, LANE), 1) < LANE // 2
    for k in range(5):
        pad[k, :, border] = jnp.where(
            left,
            pltpu.roll(pad[k, :, wide - LANE:wide], LANE - SHIFT, 1),
            pltpu.roll(pad[k, :, :LANE], SHIFT, 1),
        )

    arrive(moves[2:])
    beside = jnp.concatenate([strip_in[...], jnp.zeros((LANE - 32, tall), F32)], axis=0).T
    edge_at = LANE // 2 - REACH

    def lay(k, rows, from_west, from_east):
        at = lax.broadcasted_iota(jnp.int32, from_west.shape, 1)
        value = jnp.where(at < LANE // 2, from_east, from_west)
        pad[k, rows, border] = jnp.where(
            (at >= edge_at) & (at < edge_at + 2 * REACH), value, pad[k, rows, border]
        )

    for k in range(5):
        lay(
            k, pl.ds(0, tall), pltpu.roll(beside, LANE // 2 - 2 * k, 1),
            pltpu.roll(beside, edge_at - 16 - 2 * k, 1),
        )
        for i, rows in ((0, below), (2, above)):
            lay(
                k, rows, pltpu.roll(corner[i + 1, k], SHIFT, 1),
                pltpu.roll(corner[i, k], edge_at, 1),
            )

    @pl.when(at_edge)
    def _():
        pad[3:5, tall:tall + 1, wide:] = jnp.ones((2, 1, LANE), F32)

    first_step(border)
    new = second_step(border)
    for k in range(3):
        place_sides(k, pl.ds(0, tall), new[k][:tall])

    inputs[8].wait()

    @pl.when(at_edge)
    def _():
        place = lax.broadcasted_iota(jnp.int32, (span, obs), 0)
        place = col * wide + place - jnp.where(
            place >= wide + LANE // 2, wide + SHIFT, jnp.where(place >= wide, SHIFT - REACH - REACH, 0)
        )
        chosen_buf[...] = jnp.where(place == cells[...], 1.0, 0.0).astype(BF16)
        whole_wait(edge_in.at[pl.ds(0, slots - 1)], recv_sem.at[2]).wait_recv()
        total = edge_in[pl.ds(0, Y * X)]
        for k in range(1, depth):
            total = total + edge_in[pl.ds(k * Y * X, Y * X)]
        both_cores[core] = total
        remote(
            both_cores.at[core], both_cores.at[core], kern_sem.at[3], recv_sem.at[4], partner_core
        ).start()

    @pl.when(home)
    def _():
        whole_wait(whole_in.at[pl.ds(0, 2 * depth - 1)], recv_sem.at[3]).wait_recv()

    @pl.when(jnp.logical_not(home))
    def _():
        whole_wait(whole_in, recv_sem.at[3]).wait_recv()

    for half in range(2):
        value = whole_in[half * depth]
        for k in range(1, depth):
            value = value + whole_in[half * depth + k]
        series_buf[:, half * LANE:(half + 1) * LANE] = value

    @pl.when(at_edge)
    def _():
        whole_wait(both_cores.at[0], recv_sem.at[4]).wait_recv()
        latest = jnp.concatenate([
            both_cores[c, y_at * X + h * 2 + half]
            for y_at in range(Y) for h in range(Z_HIGH) for c in range(CORES) for half in range(2)
        ], axis=1)
        high, rest = split(latest)
        middle, rest = split(rest)
        parts = jnp.concatenate([high.astype(F32), middle.astype(F32), rest, rest], axis=0)
        picked = lax.dot_general(
            parts.astype(BF16), chosen_buf[...], (((1,), (1,)), ((), ())),
            preferred_element_type=F32,
        )
        picked = picked[0:2] + picked[2:4] + picked[4:6]
        base = tall - 2 * EDGE
        part_rows = pl.ds(base, 3 * EDGE)
        for lanes in (body, border):
            width = lanes.size
            picks = picked[:, lanes.start:lanes.start + width]
            at_ghost = lax.broadcasted_iota(jnp.int32, (3 * EDGE, width), 0) == 2 * EDGE
            ghosts = [jnp.broadcast_to(picks[k:k + 1], (3 * EDGE, width)) for k in range(2)]
            speed_sq, wet = pad[3, part_rows, lanes], pad[4, part_rows, lanes]
            face = [face_buf[k, part_rows, lanes] for k in range(4)]
            surf = jnp.where(at_ghost, ghosts[0], pad[0, part_rows, lanes])
            surf, qx, qy = step_once(
                surf, pad[1, part_rows, lanes], pad[2, part_rows, lanes], speed_sq, wet, face
            )
            surf = jnp.where(at_ghost, ghosts[1], surf)
            qx = jnp.where(at_ghost, 0.0, qx)
            qy = jnp.where(at_ghost, 0.0, qy)
            new = step_once(surf, qx, qy, speed_sq, wet, face)
            for k in range(3):
                if width == wide:
                    out_buf[k, tall - EDGE:] = new[k][EDGE:2 * EDGE]
                else:
                    place_sides(k, pl.ds(tall - EDGE, EDGE), new[k][EDGE:2 * EDGE])

    for exists, _, copy, _ in moves:
        @pl.when(exists)
        def _(copy=copy):
            copy.wait_send()
    for ref, sem in (
        (core_in, local_sem.at[0]), (late_in, local_sem.at[1]),
        (others, kern_sem.at[0]),
    ):
        whole_wait(ref, sem).wait_send()

    @pl.when(at_edge)
    def _():
        whole_wait(edge_in.at[pl.ds(0, edges - 1)], kern_sem.at[1]).wait_send()
        whole_wait(both_cores.at[0], kern_sem.at[3]).wait_send()

    @pl.when(jnp.logical_not(at_edge))
    def _():
        whole_wait(edge_in.at[pl.ds(0, edges)], kern_sem.at[1]).wait_send()

    @pl.when(home)
    def _():
        whole_wait(whole_in.at[pl.ds(0, 2 * depth - 1)], kern_sem.at[2]).wait_send()

    @pl.when(jnp.logical_not(home))
    def _():
        whole_wait(whole_in, kern_sem.at[2]).wait_send()


def write_out(series, fields, series_hbm, surf_hbm, qx_hbm, qy_hbm, sems):
    copies = [pltpu.make_async_copy(series, series_hbm, sems.at[3])]
    for k, target in enumerate((surf_hbm, qx_hbm, qy_hbm)):
        copies.append(pltpu.make_async_copy(fields.at[k], target, sems.at[k]))
    for copy in copies:
        copy.start()
    for copy in copies:
        copy.wait()


def on_device(n_rows, n_cols, kernel_hat, coefficients, wave_speed_sq, wet_mask, boundary_cell, height, flux_x, flux_y):
    _, freqs, src, obs = kernel_hat.shape
    steps = coefficients.shape[0]
    tall, wide = height.shape
    points = obs // n_cols
    own_steps = steps // n_rows
    span = wide + LANE
    forward, inverse = tables(freqs * n_rows, steps, n_rows)
    dma = pltpu.SemaphoreType.DMA
    anywhere = pl.BlockSpec(memory_space=pltpu.HBM)
    in_vmem = pl.BlockSpec(memory_space=pltpu.VMEM)
    series, fields = pl.pallas_call(
        functools.partial(kernel, n_rows, n_cols),
        out_shape=(
            pltpu.VMEM((own_steps, points), F32),
            pltpu.VMEM((3, tall, wide), F32),
        ),
        in_specs=[anywhere] * 10,
        out_specs=(in_vmem,) * 2,
        scratch_shapes=[
            pltpu.VMEM((Y, 2, freqs, src, obs // Y), BF16),
            pltpu.VMEM((src, steps), F32),
            pltpu.VMEM(forward.shape[1:], F32),
            pltpu.VMEM(inverse.shape[1:], BF16),
            pltpu.VMEM((1, obs), jnp.int32),
            pltpu.VMEM((5, tall + 2 * EDGE, span), F32),
            pltpu.VMEM((tall, wide), jnp.int32),
            pltpu.VMEM((4, 5, REACH, LANE), F32),
            pltpu.VMEM((2, 5, REACH, wide), F32),
            pltpu.VMEM((2, 5, REACH, wide), F32),
            pltpu.VMEM((32, tall), F32),
            pltpu.VMEM((32, tall), F32),
            pltpu.VMEM((Y, CORES, X, 2 * freqs, LANE), F32),
            pltpu.VMEM((Y, X, 2 * freqs, LANE), F32),
            pltpu.VMEM((Y, X, 2 * freqs, LANE), F32),
            pltpu.VMEM((Y * X, 2 * freqs, LANE), F32),
            pltpu.VMEM((X, 2 * freqs, LANE), F32),
            pltpu.VMEM((steps, LANE), F32),
            pltpu.VMEM((2 * Z_LOW * Z_HIGH, own_steps, LANE), F32),
            pltpu.VMEM((Y, CORES, X, 2, LANE), F32),
            pltpu.VMEM((Y * X * CORES - 1, 2, LANE), F32),
            pltpu.VMEM((2, LANE), F32),
            pltpu.VMEM((Z_LOW * Z_HIGH * Y * X, 2, LANE), F32),
            pltpu.VMEM((CORES, Y * X, 2, LANE), F32),
            pltpu.VMEM((4, tall + 2 * EDGE, span), F32),
            pltpu.VMEM((3, tall + 2 * EDGE, span), F32),
            pltpu.VMEM((span, obs), BF16),
            dma((5,)),
            dma((Y,)),
            dma((Y,)),
            dma((8,)),
            dma((8,)),
            dma((5,)),
            pltpu.SemaphoreType.REGULAR,
            pltpu.SemaphoreType.REGULAR,
        ],
        compiler_params=pltpu.CompilerParams(
            collective_id=0, has_side_effects=True, vmem_limit_bytes=60 * 1024 * 1024
        ),
    )(
        kernel_hat, coefficients.T, wave_speed_sq, wet_mask, boundary_cell.reshape(1, obs),
        height, flux_x, flux_y, jnp.asarray(forward), jnp.asarray(inverse),
    )
    return pl.pallas_call(
        write_out,
        out_shape=(
            jax.ShapeDtypeStruct((own_steps, points), F32),
            jax.ShapeDtypeStruct((tall, wide), F32),
            jax.ShapeDtypeStruct((tall, wide), F32),
            jax.ShapeDtypeStruct((tall, wide), F32),
        ),
        in_specs=[in_vmem] * 2,
        out_specs=(anywhere,) * 4,
        scratch_shapes=[dma((4,))],
        compiler_params=pltpu.CompilerParams(vmem_limit_bytes=4 * 1024 * 1024),
    )(series, fields)


def solution(mesh):
    n_rows, n_cols = mesh.shape["rows"], mesh.shape["cols"]
    return jax.shard_map(
        functools.partial(on_device, n_rows, n_cols),
        mesh=mesh,
        in_specs=(
            P(None, "rows", "cols", None),
            P(None, "cols"),
            P("rows", "cols"),
            P("rows", "cols"),
            P(),
            P("rows", "cols"),
            P("rows", "cols"),
            P("rows", "cols"),
        ),
        out_specs=(P("rows", "cols"), P("rows", "cols"), P("rows", "cols"), P("rows", "cols")),
        check_vma=False,
    )
```

```python
import functools
import math

import jax
import jax.numpy as jnp
import numpy as np
from jax import lax
from jax.experimental import pallas as pl
from jax.experimental.pallas import tpu as pltpu
from jax.sharding import PartitionSpec as P

MESH = pl.DeviceIdType.MESH
GROUP = 8
LANE = 128
REACH = 2
SHIFT = LANE // 2 + REACH
X, Y, Z_LOW, Z_HIGH, CORES = 4, 4, 4, 2, 2
BARRIER_AFTER = 1
EDGE = 8
F32 = jnp.float32
BF16 = jnp.bfloat16


def halves(table):
    high = table.astype(np.float32).astype(jnp.bfloat16)
    low = (table - high.astype(np.float64)).astype(np.float32).astype(jnp.bfloat16)
    return np.concatenate([high, high, low], axis=2)


def tables(freq_total, steps, row_devs):
    freq = np.arange(freq_total)
    time = np.arange(steps)
    phase = 2.0 * math.pi * (np.outer(freq, time) % freq_total) / freq_total
    cos = np.cos(phase).reshape(row_devs, -1, GROUP, steps)
    sin = np.sin(phase).reshape(row_devs, -1, GROUP, steps)
    both = np.concatenate([cos, -sin], axis=2).reshape(row_devs, -1, steps)
    forward = both.astype(np.float32)
    inverse = np.swapaxes(both, 1, 2) / freq_total
    four = np.swapaxes(both.reshape(row_devs // X, -1, steps), 1, 2) / freq_total
    late = halves(inverse[:, steps - 2 * GROUP:]).astype(np.float32)
    late = np.pad(late, ((0, 0), (0, 0), (0, steps - late.shape[2])))
    return np.concatenate([forward, late], axis=1), halves(four)


def split(value):
    high = value.astype(BF16)
    return high, value - high.astype(F32)


def faces(speed_sq, wet):
    speed = 0.0625 * jnp.sqrt(speed_sq)
    found = []
    for dim in (1, 0):
        ahead = wet.shape[dim] - 1
        opened = wet * pltpu.roll(wet, ahead, dim)
        found += [0.125 * opened, opened * (speed + pltpu.roll(speed, ahead, dim))]
    return found


def step_once(surf, qx, qy, speed_sq, wet, face):
    energy = speed_sq * surf
    change = []
    for dim, along, across, half, damp in ((1, qx, qy, *face[:2]), (0, qy, qx, *face[2:])):
        ahead = surf.shape[dim] - 1
        later = lambda v: pltpu.roll(v, ahead, dim)
        along_later = later(along)
        mass = half * (along + along_later) + damp * (surf - later(surf))
        momentum = half * (energy + later(energy)) + damp * (along - along_later)
        shear = damp * (across - later(across))
        change.append([f - pltpu.roll(f, 1, dim) for f in (mass, momentum, shear)])
    (mass_x, mom_x, shear_x), (mass_y, mom_y, shear_y) = change
    return (
        wet * (surf - (mass_x + mass_y)),
        wet * (qx - (mom_x + shear_y)),
        wet * (qy - (shear_x + mom_y)),
    )


def kernel(
    n_rows, n_cols,
    kern_hbm, coef_hbm, sq_hbm, wet_hbm, cell_hbm, surf_hbm, qx_hbm, qy_hbm, fwd_hbm, inv_hbm,
    series_buf, out_buf,
    kern, coef, fwd, inv, cells, pad, wet_int, corner, rows_out, rows_in, strip_out, strip_in,
    part, core_in, plane_out, plane_in, spec_buf, whole_buf, whole_in,
    late_part, late_in, late_out, edge_in, both_cores, face_buf, mid, chosen_buf,
    local_sem, kern_sem, core_recv, halo_send, halo_recv, recv_sem, near_sem, far_sem,
):
    row = lax.axis_index("rows")
    col = lax.axis_index("cols")
    x, z_low = lax.rem(row, X), row // X
    y, z_high, core = col // (Z_HIGH * CORES), lax.rem(col // CORES, Z_HIGH), lax.rem(col, CORES)
    z = z_high * Z_LOW + z_low
    freqs, src = kern.shape[2:4]
    groups = freqs // GROUP
    tall, wide = surf_hbm.shape
    obs = cells.shape[1]
    points = obs // n_cols
    per_y = obs // Y
    own_steps = series_buf.shape[0]
    has_n, has_s = row > 0, row < n_rows - 1
    has_w, has_e = col > 0, col < n_cols - 1
    at_edge = row == n_rows - 1

    inputs = [
        pltpu.make_async_copy(coef_hbm, coef, local_sem.at[0]),
        pltpu.make_async_copy(fwd_hbm.at[row], fwd, local_sem.at[1]),
        pltpu.make_async_copy(surf_hbm, pad.at[0, :tall, :wide], local_sem.at[3]),
        pltpu.make_async_copy(qx_hbm, pad.at[1, :tall, :wide], local_sem.at[3]),
        pltpu.make_async_copy(qy_hbm, pad.at[2, :tall, :wide], local_sem.at[3]),
        pltpu.make_async_copy(sq_hbm, pad.at[3, :tall, :wide], local_sem.at[3]),
        pltpu.make_async_copy(wet_hbm, wet_int, local_sem.at[3]),
        pltpu.make_async_copy(inv_hbm.at[z_low], inv, local_sem.at[2]),
        pltpu.make_async_copy(cell_hbm, cells, local_sem.at[4]),
    ]
    for copy in inputs[:2]:
        copy.start()
    chunks = []
    first_y = y == 0
    y_to = [
        0,
        jnp.where(first_y, 2, jnp.where(y == 1, 3, 1)),
        jnp.where(first_y, 1, jnp.where(y == 2, 3, 2)),
        jnp.where(first_y, 3, y),
    ]
    own_turn = jnp.where(first_y, 0, Y - 1)
    for i in range(Y):
        at = pl.multiple_of(y_to[i] * per_y, per_y)
        chunks.append(pltpu.make_async_copy(
            kern_hbm.at[:, :, :, pl.ds(at, per_y)], kern.at[i], kern_sem.at[i]
        ))
    chunks[0].start()
    pad[:, tall:] = jnp.zeros((5, 2 * EDGE, wide + LANE), F32)
    rows_in[...] = jnp.zeros(rows_in.shape, F32)
    strip_in[...] = jnp.zeros(strip_in.shape, F32)
    corner[...] = jnp.zeros(corner.shape, F32)

    diagonals = [
        (has_n & has_w, -1, -1), (has_n & has_e, -1, 1),
        (has_s & has_w, 1, -1), (has_s & has_e, 1, 1),
    ]
    plane = [
        (dy, dx, dc) for dy in range(Y) for dx in range(X) for dc in range(CORES) if dy or dx or dc
    ]
    depth = Z_LOW * Z_HIGH
    home = x // Z_HIGH == z_high
    barrier = pltpu.get_barrier_semaphore()

    def greet(to):
        pl.semaphore_signal(barrier, 1, device_id=to, device_id_type=MESH)

    def device(x_at, y_at, z_at, core_at):
        return (
            lax.rem(z_at, Z_LOW) * X + x_at,
            (y_at * Z_HIGH + z_at // Z_LOW) * CORES + core_at,
        )

    def in_plane(dy, dx, dc):
        return device(lax.rem(x + dx, X), lax.rem(y + dy, Y), z, lax.rem(core + dc, CORES))

    partner_core = device(x, y, z, 1 - core)

    def in_line(dz):
        return device(x, y, lax.rem(z + dz + depth, depth), core)

    for dz in (2, -2, 1, -1):
        greet(in_line(dz))
    chunks[1].start()
    for dy, dx, dc in plane:
        greet(in_plane(dy, dx, dc))
    for copy in chunks[2:]:
        copy.start()
    for copy in inputs[2:]:
        copy.start()

    def remote(source, target, send, recv, to):
        return pltpu.make_async_remote_copy(
            src_ref=source, dst_ref=target, send_sem=send, recv_sem=recv,
            device_id=to, device_id_type=MESH,
        )

    def whole_wait(ref, sem):
        return remote(ref, ref, sem, sem, partner_core)

    inputs[0].wait()
    inputs[1].wait()
    spectrum = lax.dot_general(
        fwd[:2 * freqs], coef[...], (((1,), (1,)), ((), ())),
        precision=lax.Precision.HIGHEST, preferred_element_type=F32,
    )
    spread = jnp.where(
        lax.rem(lax.broadcasted_iota(jnp.int32, (src, GROUP * src), 1), src)
        == lax.broadcasted_iota(jnp.int32, (src, GROUP * src), 0), 1.0, 0.0
    ).astype(BF16)
    shape = (2 * GROUP, GROUP * src)
    own_block = (
        lax.broadcasted_iota(jnp.int32, shape, 1) // src
        == lax.rem(lax.broadcasted_iota(jnp.int32, shape, 0), GROUP)
    )
    lefts = []
    for g in range(groups):
        mine = spectrum[g * 2 * GROUP:(g + 1) * 2 * GROUP]
        turned = jnp.concatenate([-mine[GROUP:], mine[:GROUP]], axis=0)
        for value in (mine, turned):
            tiled = jnp.dot(value.astype(BF16), spread, preferred_element_type=F32)
            lefts.append(jnp.where(own_block, tiled, 0.0).astype(BF16))

    def send_chunk(i):
        remote(
            part.at[i, 1 - core], core_in.at[i], local_sem.at[0], core_recv.at[i], partner_core
        ).start()
        ahead = lax.rem(y_to[i] - y + Y, Y) * X
        for dx in range(X):
            for dc in range(CORES):
                def send(dx=dx, dc=dc):
                    x_to, core_to = lax.rem(x + dx, X), lax.rem(core + dc, CORES)
                    remote(
                        late_part.at[i, core_to, x_to],
                        late_in.at[lax.max((ahead + dx) * CORES + dc - 1, 0)],
                        local_sem.at[1], recv_sem.at[0], device(x_to, y_to[i], z, core_to),
                    ).start()
                if dx or dc:
                    send()
                else:
                    pl.when(own_turn != i)(send)

    def gather(i):
        whole_wait(core_in.at[i], core_recv.at[i]).wait_recv()
        plane_out[i] = part[i, core] + core_in[i]
        ahead = lax.rem(y_to[i] - y + Y, Y) * X
        for dx in (2, 1, 3, 0):
            def send(dx=dx):
                x_to = lax.rem(x + dx, X)
                remote(
                    plane_out.at[i, x_to], plane_in.at[ahead + dx],
                    kern_sem.at[0], recv_sem.at[1], device(x_to, y_to[i], z, core),
                ).start()
            if dx:
                send()
            else:
                pl.when(own_turn != i)(send)

    tail = fwd[2 * freqs:].astype(BF16)[:, :6 * freqs]
    for i in range(Y):
        chunks[i].wait()
        totals = []
        for g in range(groups):
            total = None
            for p in range(2):
                right = kern[i, p, pl.ds(g * GROUP, GROUP)].reshape(GROUP * src, per_y)
                term = jnp.dot(lefts[2 * g + p], right, preferred_element_type=F32)
                total = term if total is None else total + term
            totals.append(total)
        total = jnp.concatenate(totals, axis=0)
        high, low = split(total)
        late = jnp.dot(
            tail, jnp.concatenate([high, low.astype(BF16), high], axis=0),
            preferred_element_type=F32,
        )[2 * GROUP - 2:]
        for h in range(Z_HIGH):
            for c in range(CORES):
                for half in range(2):
                    at = (h * CORES + c) * points + half * LANE
                    part[i, c, 2 * h + half] = total[:, at:at + LANE]
                    late_part[i, c, 2 * h + half] = late[:, at:at + LANE]
        if i == BARRIER_AFTER:
            pl.semaphore_wait(barrier, len(plane) + 4)
            for dz in (2, -2, 1, -1):
                pl.semaphore_signal(
                    near_sem, 1, device_id=in_line(dz), device_id_type=MESH
                )
            for j in range(i + 1):
                send_chunk(j)
        elif i > BARRIER_AFTER:
            send_chunk(i)
        if i == Y - 2:
            gather(0)

    gather(1)
    fields = pad.at[:, :tall, :wide]
    pltpu.make_async_copy(fields, fields, local_sem.at[3]).wait()
    pad[4, :tall, :wide] = wet_int[...].astype(F32)
    lane = lax.broadcasted_iota(jnp.int32, (tall, LANE), 1)
    packed = jnp.zeros((tall, LANE), F32)
    for k in range(5):
        first, last = pad[k, :tall, :LANE], pad[k, :tall, wide - LANE:wide]
        at = 2 * k
        moved = first if at == 0 else pltpu.roll(first, at, 1)
        packed = jnp.where((lane >= at) & (lane < at + 2), moved, packed)
        at = 16 + 2 * k
        packed = jnp.where(
            (lane >= at) & (lane < at + 2), pltpu.roll(last, at + 2, 1), packed
        )
    strip_out[...] = packed.T[:32]
    rows_out[0] = pad[:, :REACH, :wide]
    rows_out[1] = pad[:, tall - REACH:tall, :wide]

    gather(2)

    north = (lax.rem(row + n_rows - 1, n_rows), col)
    south = (lax.rem(row + 1, n_rows), col)
    west = (row, lax.rem(col + n_cols - 1, n_cols))
    east = (row, lax.rem(col + 1, n_cols))
    def halo(source, target, i, to):
        return remote(source, target, halo_send.at[i], halo_recv.at[i], to)

    moves = [
        (has_n, has_s, halo(rows_out.at[0], rows_in.at[0], 0, north), True),
        (has_s, has_n, halo(rows_out.at[1], rows_in.at[1], 1, south), True),
        (has_w, has_e, halo(strip_out.at[pl.ds(0, 16)], strip_in.at[pl.ds(16, 16)], 2, west), core == 1),
        (has_e, has_w, halo(strip_out.at[pl.ds(16, 16)], strip_in.at[pl.ds(0, 16)], 3, east), core == 0),
    ]
    for i, (exists, dr, dc) in enumerate(diagonals):
        side = 0 if dr < 0 else 1
        cols_at = pl.ds(0, LANE) if dc < 0 else pl.ds(wide - LANE, LANE)
        to = (lax.rem(row + dr + n_rows, n_rows), lax.rem(col + dc + n_cols, n_cols))
        moves.append((
            exists, diagonals[3 - i][0],
            halo(rows_out.at[side, :, :, cols_at], corner.at[i], 4 + i, to),
            core == (1 if dc < 0 else 0),
        ))

    def send_halos(near_ones):
        for exists, _, copy, near in moves:
            if near is True:
                if near_ones:
                    pl.when(exists)(copy.start)
            else:
                pl.when(exists & (near if near_ones else jnp.logical_not(near)))(copy.start)

    pl.semaphore_wait(near_sem, 4)
    for dz in (2, -2):
        pl.semaphore_signal(far_sem, 1, device_id=in_line(dz), device_id_type=MESH)
    send_halos(True)
    gather(Y - 1)
    pl.semaphore_wait(far_sem, 2)
    send_halos(False)

    whole_wait(late_in, recv_sem.at[0]).wait_recv()
    late = late_part[own_turn, core, x]
    for k in range(len(plane)):
        late = late + late_in[k]
    late_out[...] = late
    slot = z * (Y * X) + y * X + x
    slots = depth * Y * X
    edges = Y * Z_HIGH
    own_edge = y * Z_HIGH + z_high
    for k in range(edges):
        def _(k=k):
            to = lax.rem(own_edge + k, edges) * CORES + core
            remote(
                late_out, edge_in.at[slot], kern_sem.at[1], recv_sem.at[2], (n_rows - 1, to)
            ).start()
        if k:
            _()
        else:
            pl.when(jnp.logical_not(at_edge))(_)

    @pl.when(at_edge)
    def _():
        edge_in[slot] = late

    others = plane_in.at[pl.ds(1, X * Y - 1)]
    whole_wait(others, recv_sem.at[1]).wait_recv()
    for dx in range(X):
        value = plane_out[own_turn, x] if dx == 0 else plane_in[dx]
        for i in range(Y - 1):
            value = value + plane_in[(i + 1) * X + dx]
        spec_buf[lax.rem(x + X - dx, X)] = value
    inputs[7].wait()
    high, low = split(spec_buf[...].reshape(X * 2 * freqs, LANE))
    whole = jnp.dot(
        inv[...], jnp.concatenate([high, low.astype(BF16), high], axis=0),
        preferred_element_type=F32,
    )
    whole_buf[...] = whole
    z_base = x // 2 * Z_LOW
    own_half = lax.rem(x, 2) * depth
    for to in range(n_rows):
        @pl.when(jnp.logical_not(home & (row == to)))
        def _(to=to):
            z_to = z_base + to // X
            remote(
                whole_buf.at[pl.ds(to * own_steps, own_steps)],
                whole_in.at[own_half + lax.rem(z_to - z + depth, depth)],
                kern_sem.at[2], recv_sem.at[3], device(to % X, y, z_to, core),
            ).start()

    @pl.when(home)
    def _():
        whole_in[own_half] = whole_buf[
            pl.ds(pl.multiple_of(row * own_steps, own_steps), own_steps)
        ]

    def arrive(some):
        for _, arrives, copy, _ in some:
            @pl.when(arrives)
            def _(copy=copy):
                copy.wait_recv()

    arrive(moves[:2])
    span = wide + LANE
    below, above = pl.ds(tall, REACH), pl.ds(tall + 2 * EDGE - REACH, REACH)
    pad[:, below, :wide] = rows_in[0]
    pad[:, above, :wide] = rows_in[1]

    @pl.when(at_edge)
    def _():
        pad[3:5, tall:tall + 1, :wide] = jnp.ones((2, 1, wide), F32)

    def first_step(lanes):
        face = faces(pad[3, :, lanes], pad[4, :, lanes])
        for k in range(4):
            face_buf[k, :, lanes] = face[k]
        new = step_once(*(pad[k, :, lanes] for k in range(5)), face)
        for k in range(3):
            mid[k, :, lanes] = new[k]

    def second_step(lanes):
        face = [face_buf[k, :, lanes] for k in range(4)]
        state = [mid[k, :, lanes] for k in range(3)]
        return step_once(*state, pad[3, :, lanes], pad[4, :, lanes], face)

    def place_sides(k, rows, sides):
        at = lax.broadcasted_iota(jnp.int32, sides.shape, 1)
        first, last = pl.ds(0, LANE), pl.ds(wide - LANE, LANE)
        out_buf[k, rows, first] = jnp.where(
            at < REACH, pltpu.roll(sides, LANE - SHIFT, 1), out_buf[k, rows, first]
        )
        out_buf[k, rows, last] = jnp.where(
            at >= LANE - REACH, pltpu.roll(sides, SHIFT, 1), out_buf[k, rows, last]
        )

    body, border = pl.ds(0, wide), pl.ds(wide, LANE)
    first_step(body)
    new = second_step(body)
    for k in range(3):
        out_buf[k] = new[k][:tall]
    left = lax.broadcasted_iota(jnp.int32, (tall + 2 * EDGE, LANE), 1) < LANE // 2
    for k in range(5):
        pad[k, :, border] = jnp.where(
            left,
            pltpu.roll(pad[k, :, wide - LANE:wide], LANE - SHIFT, 1),
            pltpu.roll(pad[k, :, :LANE], SHIFT, 1),
        )

    arrive(moves[2:])
    beside = jnp.concatenate([strip_in[...], jnp.zeros((LANE - 32, tall), F32)], axis=0).T
    edge_at = LANE // 2 - REACH

    def lay(k, rows, from_west, from_east):
        at = lax.broadcasted_iota(jnp.int32, from_west.shape, 1)
        value = jnp.where(at < LANE // 2, from_east, from_west)
        pad[k, rows, border] = jnp.where(
            (at >= edge_at) & (at < edge_at + 2 * REACH), value, pad[k, rows, border]
        )

    for k in range(5):
        lay(
            k, pl.ds(0, tall), pltpu.roll(beside, LANE // 2 - 2 * k, 1),
            pltpu.roll(beside, edge_at - 16 - 2 * k, 1),
        )
        for i, rows in ((0, below), (2, above)):
            lay(
                k, rows, pltpu.roll(corner[i + 1, k], SHIFT, 1),
                pltpu.roll(corner[i, k], edge_at, 1),
            )

    @pl.when(at_edge)
    def _():
        pad[3:5, tall:tall + 1, wide:] = jnp.ones((2, 1, LANE), F32)

    first_step(border)
    new = second_step(border)
    for k in range(3):
        place_sides(k, pl.ds(0, tall), new[k][:tall])

    inputs[8].wait()

    @pl.when(at_edge)
    def _():
        place = lax.broadcasted_iota(jnp.int32, (span, obs), 0)
        place = col * wide + place - jnp.where(
            place >= wide + LANE // 2, wide + SHIFT, jnp.where(place >= wide, SHIFT - REACH - REACH, 0)
        )
        chosen_buf[...] = jnp.where(place == cells[...], 1.0, 0.0).astype(BF16)
        whole_wait(edge_in.at[pl.ds(0, slots - 1)], recv_sem.at[2]).wait_recv()
        total = edge_in[pl.ds(0, Y * X)]
        for k in range(1, depth):
            total = total + edge_in[pl.ds(k * Y * X, Y * X)]
        both_cores[core] = total
        remote(
            both_cores.at[core], both_cores.at[core], kern_sem.at[3], recv_sem.at[4], partner_core
        ).start()

    @pl.when(home)
    def _():
        whole_wait(whole_in.at[pl.ds(0, 2 * depth - 1)], recv_sem.at[3]).wait_recv()

    @pl.when(jnp.logical_not(home))
    def _():
        whole_wait(whole_in, recv_sem.at[3]).wait_recv()

    for half in range(2):
        value = whole_in[half * depth]
        for k in range(1, depth):
            value = value + whole_in[half * depth + k]
        series_buf[:, half * LANE:(half + 1) * LANE] = value

    @pl.when(at_edge)
    def _():
        whole_wait(both_cores.at[0], recv_sem.at[4]).wait_recv()
        latest = jnp.concatenate([
            both_cores[c, y_at * X + h * 2 + half]
            for y_at in range(Y) for h in range(Z_HIGH) for c in range(CORES) for half in range(2)
        ], axis=1)
        high, rest = split(latest)
        middle, rest = split(rest)
        parts = jnp.concatenate([high.astype(F32), middle.astype(F32), rest, rest], axis=0)
        picked = lax.dot_general(
            parts.astype(BF16), chosen_buf[...], (((1,), (1,)), ((), ())),
            preferred_element_type=F32,
        )
        picked = picked[0:2] + picked[2:4] + picked[4:6]
        base = tall - 2 * EDGE
        part_rows = pl.ds(base, 3 * EDGE)
        for lanes in (body, border):
            width = lanes.size
            picks = picked[:, lanes.start:lanes.start + width]
            at_ghost = lax.broadcasted_iota(jnp.int32, (3 * EDGE, width), 0) == 2 * EDGE
            ghosts = [jnp.broadcast_to(picks[k:k + 1], (3 * EDGE, width)) for k in range(2)]
            speed_sq, wet = pad[3, part_rows, lanes], pad[4, part_rows, lanes]
            face = [face_buf[k, part_rows, lanes] for k in range(4)]
            surf = jnp.where(at_ghost, ghosts[0], pad[0, part_rows, lanes])
            surf, qx, qy = step_once(
                surf, pad[1, part_rows, lanes], pad[2, part_rows, lanes], speed_sq, wet, face
            )
            surf = jnp.where(at_ghost, ghosts[1], surf)
            qx = jnp.where(at_ghost, 0.0, qx)
            qy = jnp.where(at_ghost, 0.0, qy)
            new = step_once(surf, qx, qy, speed_sq, wet, face)
            for k in range(3):
                if width == wide:
                    out_buf[k, tall - EDGE:] = new[k][EDGE:2 * EDGE]
                else:
                    place_sides(k, pl.ds(tall - EDGE, EDGE), new[k][EDGE:2 * EDGE])

    for exists, _, copy, _ in moves:
        @pl.when(exists)
        def _(copy=copy):
            copy.wait_send()
    for ref, sem in (
        (core_in, local_sem.at[0]), (late_in, local_sem.at[1]),
        (others, kern_sem.at[0]),
    ):
        whole_wait(ref, sem).wait_send()

    @pl.when(at_edge)
    def _():
        whole_wait(edge_in.at[pl.ds(0, edges - 1)], kern_sem.at[1]).wait_send()
        whole_wait(both_cores.at[0], kern_sem.at[3]).wait_send()

    @pl.when(jnp.logical_not(at_edge))
    def _():
        whole_wait(edge_in.at[pl.ds(0, edges)], kern_sem.at[1]).wait_send()

    @pl.when(home)
    def _():
        whole_wait(whole_in.at[pl.ds(0, 2 * depth - 1)], kern_sem.at[2]).wait_send()

    @pl.when(jnp.logical_not(home))
    def _():
        whole_wait(whole_in, kern_sem.at[2]).wait_send()


def write_out(series, fields, series_hbm, surf_hbm, qx_hbm, qy_hbm, sems):
    copies = [pltpu.make_async_copy(series, series_hbm, sems.at[3])]
    for k, target in enumerate((surf_hbm, qx_hbm, qy_hbm)):
        copies.append(pltpu.make_async_copy(fields.at[k], target, sems.at[k]))
    for copy in copies:
        copy.start()
    for copy in copies:
        copy.wait()


def on_device(n_rows, n_cols, kernel_hat, coefficients, wave_speed_sq, wet_mask, boundary_cell, height, flux_x, flux_y):
    _, freqs, src, obs = kernel_hat.shape
    steps = coefficients.shape[0]
    tall, wide = height.shape
    points = obs // n_cols
    own_steps = steps // n_rows
    span = wide + LANE
    forward, inverse = tables(freqs * n_rows, steps, n_rows)
    dma = pltpu.SemaphoreType.DMA
    anywhere = pl.BlockSpec(memory_space=pltpu.HBM)
    in_vmem = pl.BlockSpec(memory_space=pltpu.VMEM)
    series, fields = pl.pallas_call(
        functools.partial(kernel, n_rows, n_cols),
        out_shape=(
            pltpu.VMEM((own_steps, points), F32),
            pltpu.VMEM((3, tall, wide), F32),
        ),
        in_specs=[anywhere] * 10,
        out_specs=(in_vmem,) * 2,
        scratch_shapes=[
            pltpu.VMEM((Y, 2, freqs, src, obs // Y), BF16),
            pltpu.VMEM((src, steps), F32),
            pltpu.VMEM(forward.shape[1:], F32),
            pltpu.VMEM(inverse.shape[1:], BF16),
            pltpu.VMEM((1, obs), jnp.int32),
            pltpu.VMEM((5, tall + 2 * EDGE, span), F32),
            pltpu.VMEM((tall, wide), jnp.int32),
            pltpu.VMEM((4, 5, REACH, LANE), F32),
            pltpu.VMEM((2, 5, REACH, wide), F32),
            pltpu.VMEM((2, 5, REACH, wide), F32),
            pltpu.VMEM((32, tall), F32),
            pltpu.VMEM((32, tall), F32),
            pltpu.VMEM((Y, CORES, X, 2 * freqs, LANE), F32),
            pltpu.VMEM((Y, X, 2 * freqs, LANE), F32),
            pltpu.VMEM((Y, X, 2 * freqs, LANE), F32),
            pltpu.VMEM((Y * X, 2 * freqs, LANE), F32),
            pltpu.VMEM((X, 2 * freqs, LANE), F32),
            pltpu.VMEM((steps, LANE), F32),
            pltpu.VMEM((2 * Z_LOW * Z_HIGH, own_steps, LANE), F32),
            pltpu.VMEM((Y, CORES, X, 2, LANE), F32),
            pltpu.VMEM((Y * X * CORES - 1, 2, LANE), F32),
            pltpu.VMEM((2, LANE), F32),
            pltpu.VMEM((Z_LOW * Z_HIGH * Y * X, 2, LANE), F32),
            pltpu.VMEM((CORES, Y * X, 2, LANE), F32),
            pltpu.VMEM((4, tall + 2 * EDGE, span), F32),
            pltpu.VMEM((3, tall + 2 * EDGE, span), F32),
            pltpu.VMEM((span, obs), BF16),
            dma((5,)),
            dma((Y,)),
            dma((Y,)),
            dma((8,)),
            dma((8,)),
            dma((5,)),
            pltpu.SemaphoreType.REGULAR,
            pltpu.SemaphoreType.REGULAR,
        ],
        compiler_params=pltpu.CompilerParams(
            collective_id=0, has_side_effects=True, vmem_limit_bytes=60 * 1024 * 1024
        ),
    )(
        kernel_hat, coefficients.T, wave_speed_sq, wet_mask, boundary_cell.reshape(1, obs),
        height, flux_x, flux_y, jnp.asarray(forward), jnp.asarray(inverse),
    )
    return pl.pallas_call(
        write_out,
        out_shape=(
            jax.ShapeDtypeStruct((own_steps, points), F32),
            jax.ShapeDtypeStruct((tall, wide), F32),
            jax.ShapeDtypeStruct((tall, wide), F32),
            jax.ShapeDtypeStruct((tall, wide), F32),
        ),
        in_specs=[in_vmem] * 2,
        out_specs=(anywhere,) * 4,
        scratch_shapes=[dma((4,))],
        compiler_params=pltpu.CompilerParams(vmem_limit_bytes=4 * 1024 * 1024),
    )(series, fields)


def solution(mesh):
    n_rows, n_cols = mesh.shape["rows"], mesh.shape["cols"]
    return jax.shard_map(
        functools.partial(on_device, n_rows, n_cols),
        mesh=mesh,
        in_specs=(
            P(None, "rows", "cols", None),
            P(None, "cols"),
            P("rows", "cols"),
            P("rows", "cols"),
            P(),
            P("rows", "cols"),
            P("rows", "cols"),
            P("rows", "cols"),
        ),
        out_specs=(P("rows", "cols"), P("rows", "cols"), P("rows", "cols"), P("rows", "cols")),
        check_vma=False,
    )
```
